512 devices in a mesh: section: 8 (over y), freq: 64 (over z, x, core).
Axes of the slice: x: 4, y: 8, z: 8, core: 2. Of those that a mesh axis runs over, the one named last changes fastest.
Arguments:
- spectra: float32 [16, 16, 524288], P('section', None, 'freq'), may hold values from 0.1 to 90, as said below
- channel_gain: float32 [524288], P('freq'), may hold values from 0.5 to 2
- bandpass_bin: int32 [524288], P('freq'), may hold values from 0 to 255, never falling along the last dimension, each value on 1 to 8192 neighbouring positions
- drift_range: int32 [16], replicated, may hold values from 1 to 8, as said below
- hit_cutoff: int32 [16, 8, 16], replicated, may hold values from 0 to 1023
Outputs:
- drift_score: float32 [16, 8, 524288], P(None, 'section', 'freq')
The draws below stay inside these ranges and needn't reach their ends.
Inputs may be any that keep to these rules, and one draw needn't show every extreme that they name: `spectra`: every entry is positive. `bandpass_bin`: the bins never fall along the channels and each of the 256 bins holds 1 to 8192 channels. `drift_range`: some group reaches 8 and some other group searches stride 1 only.
All inputs are finite; a program needn't handle non-finite values.
Results may differ from the reference program's by a relative error of at most 0.0003.
Values sent between devices are 32-bit elements; how exact they have to be, the bound alone decides.
A program may use at most 64 MiB of HBM per device.

```python
import math
import jax
import jax.numpy as jnp
import numpy as np
from jax import lax

INTEG = 16
F_DEV = 8192
KMAX = 8
CHANNELS = 524288
GROUPS = 16
BINS = 256


def draw_spectra(key, part):
    first_key, second_key = jax.random.split(jax.random.fold_in(key, 11))
    group_ramp = 1.0 + 2.0 * jnp.arange(GROUPS, dtype=jnp.float32) / max(GROUPS - 1, 1)
    chan_ramp = 1.0 + 2.0 * jnp.arange(CHANNELS, dtype=jnp.float32) / (CHANNELS - 1)
    channel_scale = jnp.exp(jax.random.uniform(first_key, (GROUPS, 1, CHANNELS), jnp.float32, -1.2, 1.2))
    element = jax.random.uniform(second_key, (GROUPS, INTEG, CHANNELS), jnp.float32, 0.5, 1.5)
    result_array = channel_scale * element * group_ramp[:, None, None] * chan_ramp[None, None, :]
    return result_array.astype(jnp.float32)


def draw_drift_range(key, part):
    reach_all = jax.random.randint(jax.random.fold_in(key, 21), (GROUPS,), 1, KMAX + 1).astype(jnp.int32)
    chosen = jax.random.randint(jax.random.fold_in(key, 22), (), 0, GROUPS).astype(jnp.int32)
    step_over = jax.random.randint(jax.random.fold_in(key, 23), (), 1, GROUPS).astype(jnp.int32)
    lowest = (chosen + step_over) % GROUPS
    reach_all = reach_all.at[chosen].set(KMAX)
    reach_all = reach_all.at[lowest].set(1)
    return reach_all.astype(jnp.int32)


def place_ends(array, key, smallest, top_value):
    longest = array.shape.index(max(array.shape))
    spots = []
    for shift in (0, 1):
        where = [jax.random.randint(jax.random.fold_in(key, axis), (), 0, length) for axis, length in enumerate(array.shape)]
        where[longest] = (where[longest] + shift) % array.shape[longest]
        spots.append(tuple(where))
    return array.at[spots[0]].set(smallest).at[spots[1]].set(top_value)


def block_levels(rng, extent, pieces, low, top_value):
    level = 1.0
    for dim, shards_of in pieces:
        draws = jax.random.uniform(jax.random.fold_in(jax.random.fold_in(rng, 6), dim), (shards_of,), jnp.float32, low / len(pieces), top_value / len(pieces))
        level = level * jnp.repeat(jnp.exp(draws), extent[dim] // shards_of).reshape((-1,) + (1,) * (len(extent) - 1 - dim))
    return level


def split_up(amount, total, reach, lean):
    weights = [(1 << 20) // math.isqrt(grade ** lean) + 1 for grade in range(2, amount + 1)]
    rest, counts = total - reach - (amount - 1), [1] * (amount - 1)
    while rest > 0:
        movable = [i for i in range(amount - 1) if counts[i] < reach]
        pool, left = sum([weights[i] for i in movable]), rest
        for i in movable:
            addition = min(reach - counts[i], max(1, left * weights[i] // pool), rest)
            counts[i] = counts[i] + addition
            rest = rest - addition
    return np.array([reach] + counts)


def uneven_parts(own_key, amount, total, reach, lean):
    if amount == 2:
        one = jax.random.randint(own_key, (), max(1, total - reach), min(reach, total - 1) + 1)
        return jnp.stack([one, total - one])
    lengths = jnp.asarray(split_up(amount, total, reach, lean), jnp.int32)
    twos = (amount - 1) // 2
    giver, sink = lengths[1:1 + 2 * twos:2], lengths[2:2 + 2 * twos:2]
    slack = jnp.minimum(giver - 1, reach - sink)
    shifted = jax.random.randint(jax.random.fold_in(own_key, 1), (twos,), 0, 1 << 20) % (slack + 1)
    lengths = lengths.at[1:1 + 2 * twos:2].set(giver - shifted).at[2:2 + 2 * twos:2].set(sink + shifted)
    return lengths[jax.random.permutation(jax.random.fold_in(own_key, 2), amount)]


def setup_inputs(seed: int = 0) -> dict:
    key_of = jax.random.split(jax.random.key(seed), 6)
    return {
        "spectra": draw_spectra(jax.random.fold_in(key_of[5], 71), 0),
        "channel_gain": jnp.clip(jnp.exp(math.log(2.0) - 1.3862944 * jax.random.uniform(key_of[1], (CHANNELS,), jnp.float32) ** block_levels(key_of[1], (CHANNELS,), ((0, 64),), -0.2, 0.2)), 0.5, 2.0),
        "bandpass_bin": jnp.searchsorted(jnp.cumsum(uneven_parts(key_of[2], BINS, CHANNELS, F_DEV, 0)), jnp.arange(CHANNELS), side="right").astype(jnp.int32),
        "drift_range": draw_drift_range(jax.random.fold_in(key_of[5], 71), 0),
        "hit_cutoff": place_ends(jax.random.randint(key_of[4], (GROUPS, KMAX, INTEG), 0, 1024), jax.random.fold_in(key_of[4], 1), 0, 1023).astype(jnp.int32),
    }


def taylor_tree(extended, stride, margin):
    length = extended.shape[-1]
    current = extended[:, None, :]
    blocks_width = 1
    while current.shape[0] > 1:
        former = current[0::2]
        latter = jnp.pad(current[1::2], ((0, 0), (0, 0), (0, margin)))
        merged = []
        for half_idx in range(blocks_width):
            anchor = former[:, half_idx]
            source = latter[:, half_idx]
            merged.append(anchor + lax.dynamic_slice_in_dim(source, half_idx * stride, length, axis=1))
            merged.append(anchor + lax.dynamic_slice_in_dim(source, (half_idx + 1) * stride, length, axis=1))
        current = jnp.stack(merged, axis=1)
        blocks_width = blocks_width * 2
    return current[0]


def score_rate(extended, stride, cut_row, chan_dev, margin):
    drifts = taylor_tree(extended, stride, margin)[:, :chan_dev]
    cut_levels = cut_row.astype(jnp.float32) / 256.0
    return jnp.mean(jax.nn.relu(0.25 * drifts - cut_levels[:, None]), axis=0)


def reference(spectra, channel_gain, bandpass_bin, drift_range, hit_cutoff):
    calibrated = spectra * channel_gain[None, None, :]
    summed = jnp.sum(calibrated, axis=1)
    bin_sums = jax.ops.segment_sum(summed.T, bandpass_bin, num_segments=BINS, indices_are_sorted=True).T
    tally_row = jax.ops.segment_sum(jnp.full(bandpass_bin.shape, float(INTEG), jnp.float32), bandpass_bin, num_segments=BINS, indices_are_sorted=True)
    tallies = jnp.broadcast_to(tally_row[None, :], bin_sums.shape)
    running = jnp.cumsum(bin_sums, axis=0) / jnp.cumsum(tallies, axis=0)
    levels = jnp.take(running, bandpass_bin, axis=1)
    normal = calibrated / levels[:, None, :] - 1.0
    margin = KMAX * (INTEG - 1)

    def per_group(group_items):
        data_rows, reach_max, cut_rows = group_items
        extended = jnp.pad(data_rows, ((0, 0), (0, margin)))
        rate_rows = []
        for stride in range(1, KMAX + 1):
            rate_rows.append(lax.cond(stride <= reach_max,
                                      lambda: score_rate(extended, stride, cut_rows[stride - 1], CHANNELS, margin),
                                      lambda: jnp.zeros((CHANNELS,), jnp.float32)))
        return jnp.stack(rate_rows)

    return lax.map(per_group, (normal, drift_range, hit_cutoff))
```

```python
import functools

import jax
import jax.numpy as jnp
from jax import lax
from jax.experimental import pallas as pl
from jax.experimental.pallas import tpu as pltpu
from jax.sharding import PartitionSpec as P

F32 = jnp.float32
BF16 = jnp.bfloat16
LANES = 128
SUB = 8
MESH = pl.DeviceIdType.MESH


def remote(src, dst, send, recv, where):
    return pltpu.make_async_remote_copy(
        src_ref=src, dst_ref=dst, send_sem=send, recv_sem=recv, device_id=where, device_id_type=MESH
    )


def kernel(
    sizes,
    spec_hbm,
    gain_hbm,
    bins_hbm,
    reach_hbm,
    cut_hbm,
    out_ref,
    nat,
    gain,
    bins,
    reach,
    cut,
    halo,
    halo_gain,
    halo_bins,
    ext_gain,
    ext_bins,
    norm,
    quads,
    scores,
    part,
    near,
    near_sum,
    far,
    far_sum,
    early,
    load_sem,
    near_send,
    near_recv,
    far_send,
    far_recv,
    early_send,
    early_recv,
    halo_send,
    halo_recv,
    score_send,
    score_recv,
):
    ns, nf, nc, groups, integ, chans, total_bins = sizes
    nz = nf // nc
    width = chans // SUB
    cols = width // LANES
    rows = chans // LANES
    me = lax.axis_index("section")
    here = lax.axis_index("freq")
    z, xc = here // nc, here % nc

    near_peers = [z * nc + (xc + d) % nc for d in range(1, nc)]
    far_peers = [((z + d) % nz) * nc + xc for d in range(1, nz)]
    section_peers = [(me + d) % ns for d in range(1, ns)]
    left, right = (here + nf - 1) % nf, (here + 1) % nf

    loads = [
        pltpu.make_async_copy(bins_hbm, bins, load_sem.at[0]),
        pltpu.make_async_copy(gain_hbm, gain, load_sem.at[1]),
    ]
    loads += [
        pltpu.make_async_copy(spec_hbm.at[g], nat.at[g], load_sem.at[2 + g]) for g in range(groups)
    ]
    loads += [
        pltpu.make_async_copy(reach_hbm, reach, load_sem.at[2 + groups]),
        pltpu.make_async_copy(cut_hbm.at[pl.ds(groups * me, groups)], cut, load_sem.at[3 + groups]),
    ]
    for c in loads:
        c.start()

    barrier = pltpu.get_barrier_semaphore()
    for peer in near_peers + far_peers + [left, right]:
        pl.semaphore_signal(barrier, inc=1, device_id={"freq": peer}, device_id_type=MESH)
    for peer in section_peers:
        pl.semaphore_signal(barrier, inc=1, device_id={"section": peer}, device_id_type=MESH)

    for c in loads[: 2 + groups]:
        c.wait()
    acc = jnp.zeros((SUB, total_bins), F32)
    step = min(8, rows)
    bin_row = lax.broadcasted_iota(jnp.int32, (total_bins, LANES), 0)
    for r0 in range(0, rows, step):
        one_hot = jnp.concatenate(
            [(bin_row == bins[r : r + 1, :]).astype(F32).astype(BF16) for r in range(r0, r0 + step)],
            axis=1,
        )
        gain_row = jnp.concatenate([gain[r : r + 1, :] for r in range(r0, r0 + step)], axis=1)
        span = pl.ds(r0 * LANES, step * LANES)
        value = jnp.concatenate(
            [jnp.sum(nat[g, :, span], axis=0, keepdims=True) for g in range(groups)], axis=0
        )
        value = value * gain_row
        high = value.astype(BF16)
        rest = value - high.astype(F32)
        middle = rest.astype(BF16)
        low = rest - middle.astype(F32)
        lhs = jnp.concatenate(
            [high.astype(F32), middle.astype(F32), low, jnp.ones_like(value)], axis=0
        )
        acc = acc + lax.dot_general(
            lhs.astype(BF16), one_hot, (((1,), (1,)), ((), ())), preferred_element_type=F32
        )
    sums = acc[0:2] + acc[2:4] + acc[4:6]
    counts = acc[6:8]
    tile = jnp.concatenate(
        [sums[:, :LANES], counts[:, :LANES], sums[:, LANES:], counts[:, LANES:]], axis=0
    )
    part[...] = tile

    pl.semaphore_wait(barrier, nc + nz + ns - 1)

    near_copies = [
        remote(part, near.at[d], near_send.at[d], near_recv.at[d], {"freq": p})
        for d, p in enumerate(near_peers)
    ]
    halo_copies = [
        remote(src, dst, halo_send.at[i], halo_recv.at[i], {"freq": left})
        for i, (src, dst) in enumerate(
            [
                (nat.at[:, :, pl.ds(0, LANES)], halo),
                (gain.at[pl.ds(0, SUB)], halo_gain),
                (bins.at[pl.ds(0, SUB)], halo_bins),
            ]
        )
    ]
    for c in near_copies + halo_copies:
        c.start()

    def relay(g):
        for o in range(integ // SUB):
            slab = nat[g, o * SUB : (o + 1) * SUB, :]
            turned = jnp.transpose(
                jnp.stack([slab[:, s * width : (s + 1) * width] for s in range(SUB)]), (1, 0, 2)
            )
            for j in range(cols):
                norm[g, pl.ds(o * SUB, SUB), j] = turned[:, :, j * LANES : (j + 1) * LANES]

    relay(0)
    for c in near_copies:
        c.wait_recv()
    near_tile = tile
    for d in range(nc - 1):
        near_tile = near_tile + near[d]
    near_sum[...] = near_tile
    far_copies = [
        remote(near_sum, far.at[d], far_send.at[d], far_recv.at[d], {"freq": p})
        for d, p in enumerate(far_peers)
    ]
    for c in far_copies:
        c.start()

    for g in range(1, groups):
        relay(g)
    for c in far_copies:
        c.wait_recv()
    far_tile = near_tile
    for d in range(nz - 1):
        far_tile = far_tile + far[d]
    far_sum[...] = far_tile
    early_copies = [
        remote(far_sum, early.at[d], early_send.at[d], early_recv.at[d], {"section": p})
        for d, p in enumerate(section_peers)
    ]
    for c in early_copies:
        c.start()

    for c in halo_copies:
        c.wait_recv()
    sub = lax.broadcasted_iota(jnp.int32, (SUB, LANES), 0)
    last = sub == SUB - 1

    def past(first, row):
        return jnp.where(last, jnp.broadcast_to(row, (SUB, LANES)), pltpu.roll(first, SUB - 1, 0))

    for j in range(cols):
        ext_gain[j] = gain[pl.ds(j, SUB, stride=cols), :]
        ext_bins[j] = bins[pl.ds(j, SUB, stride=cols), :]
    ext_gain[cols] = past(ext_gain[0], halo_gain[0:1, :])
    ext_bins[cols] = past(ext_bins[0], halo_bins[0:1, :])
    for g in range(groups):
        for t in range(integ):
            norm[g, t, cols] = past(norm[g, t, 0], halo[g, t : t + 1, :])

    for c in loads[2 + groups :]:
        c.wait()
    for c in early_copies:
        c.wait_recv()
    before = jnp.zeros((SUB, LANES), F32)
    for d in range(1, ns):
        before = before + jnp.where(d <= me, early[d - 1], 0.0)
    run_low = before[0:1] + before[1:2]
    run_high = before[4:5] + before[5:6]
    wanted = jnp.logical_not(jnp.logical_and(last, here == nf - 1))
    for g in range(groups):
        run_low = run_low + far_tile[g : g + 1]
        run_high = run_high + far_tile[4 + g : 5 + g]
        order = (integ * (groups * me + g + 1)).astype(F32)
        table_low = jnp.broadcast_to(order * far_tile[2:3] / run_low, (SUB, LANES))
        table_high = jnp.broadcast_to(order * far_tile[6:7] / run_high, (SUB, LANES))
        factor = []
        for j in range(cols + 1):
            at = ext_bins[j]
            inner = jnp.bitwise_and(at, LANES - 1)
            inverse = jnp.where(
                at < LANES,
                jnp.take_along_axis(table_low, inner, axis=1),
                jnp.take_along_axis(table_high, inner, axis=1),
            )
            factor.append(ext_gain[j] * inverse)
        for t in range(integ):
            for j in range(cols):
                norm[g, t, j] = norm[g, t, j] * factor[j] - 1.0
            norm[g, t, cols] = jnp.where(wanted, norm[g, t, cols] * factor[cols] - 1.0, 0.0)

    lane = lax.broadcasted_iota(jnp.int32, (1, SUB, LANES), 2)

    def score_copy(i, dst):
        return remote(
            scores.at[i],
            out_ref.at[pl.ds(groups * me, groups)],
            score_send.at[i],
            score_recv.at[i],
            {"section": dst},
        )

    def target(i):
        m, r = i // 2, i % 2
        return (me + ns // 2 + m - r * (2 * m + 1)) % ns

    def one_stride(i, carry):
        dst = target(i)
        stride = dst + 1
        inside = [lane < LANES - n * stride for n in range(integ // 2 + 1)]

        def shifted(x, n):
            if n == 0:
                return x
            turned = pltpu.roll(x, LANES - n * stride, 2)
            kept = jnp.where(inside[n], turned[:cols], turned[1:])
            return jnp.concatenate([kept, turned[cols:]], axis=0)

        for g in range(groups):
            for q in range(integ // 4):
                x0, x1, x2, x3 = (norm[g, 4 * q + t] for t in range(4))
                u0, u1 = x0 + x1, x0 + shifted(x1, 1)
                v0, v1 = x2 + x3, x2 + shifted(x3, 1)
                quads[g, 4 * q] = u0 + v0
                quads[g, 4 * q + 1] = u0 + shifted(v0, 1)
                quads[g, 4 * q + 2] = u1 + shifted(v1, 1)
                quads[g, 4 * q + 3] = u1 + shifted(v1, 2)
            total = jnp.zeros((cols, SUB, LANES), F32)
            for h in range(integ // 2):
                a = h // 2
                first = quads[g, a] + shifted(quads[g, 4 + a], h - a)
                second = quads[g, 8 + a] + shifted(quads[g, 12 + a], h - a)
                for d in (2 * h, 2 * h + 1):
                    level = cut[g, dst, d].astype(F32) * (4.0 / 256.0)
                    drift = first[:cols] + shifted(second, d - h)[:cols]
                    total = total + jnp.maximum(drift - level, 0.0)
            weight = jnp.where(stride <= reach[groups * me + g], 0.25 / integ, 0.0)
            total = total * weight
            for j in range(cols):
                scores[i, g, pl.ds(j, SUB, stride=cols), :] = total[j]

        @pl.when(i < ns - 1)
        def _():
            score_copy(i, dst).start()

        return carry

    lax.fori_loop(0, ns, one_stride, 0)
    out_ref[pl.ds(groups * me, groups)] = scores[ns - 1]
    for i in range(ns - 1):
        score_copy(i, target(i)).wait_recv()
    for c in near_copies + halo_copies + far_copies + early_copies:
        c.wait_send()
    for i in range(ns - 1):
        score_copy(i, target(i)).wait_send()


def shards(near_count, spectra, channel_gain, bandpass_bin, drift_range, hit_cutoff):
    groups, integ, chans = spectra.shape
    ns, nf = lax.axis_size("section"), lax.axis_size("freq")
    total_bins = 2 * LANES
    nc, nz = near_count, nf // near_count
    rows, cols = chans // LANES, chans // LANES // SUB
    sizes = (ns, nf, nc, groups, integ, chans, total_bins)
    dma = pltpu.SemaphoreType.DMA
    tile = (SUB, LANES)
    out = pl.pallas_call(
        functools.partial(kernel, sizes),
        out_shape=jax.ShapeDtypeStruct((ns * groups, rows, LANES), F32),
        in_specs=[pl.BlockSpec(memory_space=pl.ANY)] * 5,
        out_specs=pl.BlockSpec(memory_space=pltpu.VMEM),
        scratch_shapes=[
            pltpu.VMEM((groups, integ, chans), F32),
            pltpu.VMEM((rows, LANES), F32),
            pltpu.VMEM((rows, LANES), jnp.int32),
            pltpu.SMEM((ns * groups,), jnp.int32),
            pltpu.SMEM((groups, *hit_cutoff.shape[1:]), jnp.int32),
            pltpu.VMEM((groups, integ, LANES), F32),
            pltpu.VMEM(tile, F32),
            pltpu.VMEM(tile, jnp.int32),
            pltpu.VMEM((cols + 1, *tile), F32),
            pltpu.VMEM((cols + 1, *tile), jnp.int32),
            pltpu.VMEM((groups, integ, cols + 1, *tile), F32),
            pltpu.VMEM((groups, integ, cols + 1, *tile), F32),
            pltpu.VMEM((ns, groups, rows, LANES), F32),
            pltpu.VMEM(tile, F32),
            pltpu.VMEM((max(nc - 1, 1), *tile), F32),
            pltpu.VMEM(tile, F32),
            pltpu.VMEM((max(nz - 1, 1), *tile), F32),
            pltpu.VMEM(tile, F32),
            pltpu.VMEM((ns - 1, *tile), F32),
            dma((4 + groups,)),
            dma((max(nc - 1, 1),)),
            dma((max(nc - 1, 1),)),
            dma((max(nz - 1, 1),)),
            dma((max(nz - 1, 1),)),
            dma((ns - 1,)),
            dma((ns - 1,)),
            dma((3,)),
            dma((3,)),
            dma((ns - 1,)),
            dma((ns - 1,)),
        ],
        compiler_params=pltpu.CompilerParams(collective_id=0, has_side_effects=True),
    )(
        spectra,
        channel_gain.reshape(rows, LANES),
        bandpass_bin.reshape(rows, LANES),
        drift_range,
        hit_cutoff,
    )
    return out.reshape(ns * groups, 1, chans)


def solution(mesh, near_count=8):
    return jax.shard_map(
        functools.partial(shards, near_count),
        mesh=mesh,
        in_specs=(P("section", None, "freq"), P("freq"), P("freq"), P(), P()),
        out_specs=P(None, "section", "freq"),
        check_vma=False,
    )
```

```python
import functools

import jax
import jax.numpy as jnp
from jax import lax
from jax.experimental import pallas as pl
from jax.experimental.pallas import tpu as pltpu
from jax.sharding import PartitionSpec as P

F32 = jnp.float32
BF16 = jnp.bfloat16
LANES = 128
SUB = 8
MESH = pl.DeviceIdType.MESH


def remote(src, dst, send, recv, where):
    return pltpu.make_async_remote_copy(
        src_ref=src, dst_ref=dst, send_sem=send, recv_sem=recv, device_id=where, device_id_type=MESH
    )


def kernel(
    sizes,
    spec_hbm,
    gain_hbm,
    bins_hbm,
    reach_hbm,
    cut_hbm,
    out_ref,
    nat,
    gain,
    bins,
    reach,
    cut,
    halo,
    halo_gain,
    halo_bins,
    factor,
    factor_rows,
    norm,
    quads,
    total,
    scores,
    part,
    near,
    near_sum,
    far,
    far_sum,
    early,
    spec_sem,
    load_sem,
    near_send,
    near_recv,
    far_send,
    far_recv,
    early_send,
    early_recv,
    halo_send,
    halo_recv,
    score_send,
    score_recv,
):
    ns, nf, nc, groups, integ, chans, total_bins = sizes
    nz = nf // nc
    rows = chans // LANES
    wide = groups * rows
    me = lax.axis_index("section")
    here = lax.axis_index("freq")
    z, xc = here // nc, here % nc

    near_peers = [z * nc + (xc + d) % nc for d in range(1, nc)]
    far_peers = [((z + d) % nz) * nc + xc for d in range(1, nz)]
    section_peers = [(me + d) % ns for d in range(1, ns)]
    left, right = (here + nf - 1) % nf, (here + 1) % nf

    loads = [
        pltpu.make_async_copy(bins_hbm, bins, load_sem.at[0]),
        pltpu.make_async_copy(gain_hbm, gain, load_sem.at[1]),
        pltpu.make_async_copy(reach_hbm, reach, load_sem.at[2]),
        pltpu.make_async_copy(cut_hbm.at[pl.ds(groups * me, groups)], cut, load_sem.at[3]),
    ]
    spec_loads = [
        pltpu.make_async_copy(
            spec_hbm.at[g, t // SUB, :, t % SUB, :],
            nat.at[g, t, pl.ds(0, rows)],
            spec_sem.at[g * integ + t],
        )
        for g in range(groups)
        for t in range(integ)
    ]
    for c in loads[:2] + spec_loads + loads[2:]:
        c.start()

    barrier = pltpu.get_barrier_semaphore()
    for peer in near_peers + far_peers + [left, right]:
        pl.semaphore_signal(barrier, inc=1, device_id={"freq": peer}, device_id_type=MESH)
    for peer in section_peers:
        pl.semaphore_signal(barrier, inc=1, device_id={"section": peer}, device_id_type=MESH)

    bin_row = lax.broadcasted_iota(jnp.int32, (total_bins, LANES), 0)
    for c in loads[:2]:
        c.wait()
    for c in spec_loads:
        c.wait()
    acc = jnp.zeros((SUB, total_bins), F32)
    for r0 in range(0, rows, SUB):
        span = pl.ds(r0, SUB)
        high, middle, low = [], [], []
        for g in range(groups):
            value = nat[g, 0, span]
            for t in range(1, integ):
                value = value + nat[g, t, span]
            value = value * gain[span]
            high.append(value.astype(BF16).astype(F32))
            value = value - high[-1]
            middle.append(value.astype(BF16).astype(F32))
            low.append(value - middle[-1])
        ones = [jnp.ones((SUB, LANES), F32)] * 2
        turned = jnp.transpose(jnp.stack(high + middle + low + ones), (1, 0, 2))
        lhs = jnp.concatenate([turned[r] for r in range(SUB)], axis=1).astype(BF16)
        one_hot = jnp.concatenate(
            [
                (bin_row == bins[r : r + 1, :]).astype(F32).astype(BF16)
                for r in range(r0, r0 + SUB)
            ],
            axis=1,
        )
        acc = acc + lax.dot_general(
            lhs,
            one_hot,
            (((1,), (1,)), ((), ())),
            preferred_element_type=F32,
        )
    sums = acc[0:2] + acc[2:4] + acc[4:6]
    counts = acc[6:8]
    tile = jnp.concatenate(
        [sums[:, :LANES], counts[:, :LANES], sums[:, LANES:], counts[:, LANES:]], axis=0
    )
    part[...] = tile

    pl.semaphore_wait(barrier, nc + nz + ns - 1)

    near_copies = [
        remote(part, near.at[d], near_send.at[d], near_recv.at[d], {"freq": p})
        for d, p in enumerate(near_peers)
    ]
    halo_copies = [
        remote(src, dst, halo_send.at[i], halo_recv.at[i], {"freq": left})
        for i, (src, dst) in enumerate(
            [
                (nat.at[:, :, 0], halo),
                (gain.at[pl.ds(0, SUB)], halo_gain),
                (bins.at[pl.ds(0, SUB)], halo_bins),
            ]
        )
    ]
    for c in near_copies + halo_copies:
        c.start()

    def turn(t, shift):
        block = jnp.concatenate(
            [nat[g, t, pl.ds(shift, rows)] for g in range(groups)], axis=0
        )
        norm[t, pl.ds(shift * LANES, LANES)] = jnp.transpose(block)

    for t in range(integ):
        turn(t, 0)
    for c in near_copies:
        c.wait_recv()
    near_tile = tile
    for d in range(nc - 1):
        near_tile = near_tile + near[d]
    near_sum[...] = near_tile
    far_copies = [
        remote(near_sum, far.at[d], far_send.at[d], far_recv.at[d], {"freq": p})
        for d, p in enumerate(far_peers)
    ]
    for c in far_copies:
        c.start()

    for c in halo_copies:
        c.wait_recv()
    for g in range(groups):
        for t in range(integ):
            nat[g, t, pl.ds(rows, 1)] = halo[g, t : t + 1]
    for t in range(integ):
        turn(t, 1)

    for c in far_copies:
        c.wait_recv()
    far_tile = near_tile
    for d in range(nz - 1):
        far_tile = far_tile + far[d]
    far_sum[...] = far_tile
    early_copies = [
        remote(far_sum, early.at[d], early_send.at[d], early_recv.at[d], {"section": p})
        for d, p in enumerate(section_peers)
    ]
    for c in early_copies:
        c.start()

    for c in loads[2:]:
        c.wait()
    lane = lax.broadcasted_iota(jnp.int32, (SUB, wide), 1)
    ends = jnp.logical_and(lane % rows == rows - 1, here == nf - 1)
    ones_past = jnp.where(ends, 0.0, 1.0)[0:1]
    for c in early_copies:
        c.wait_recv()
    before = jnp.zeros((SUB, LANES), F32)
    for d in range(1, ns):
        before = before + jnp.where(d <= me, early[d - 1], 0.0)
    run_low = before[0:1] + before[1:2]
    run_high = before[4:5] + before[5:6]

    def looked_up(at, low, high):
        inner = jnp.bitwise_and(at, LANES - 1)
        return jnp.where(
            at < LANES,
            jnp.take_along_axis(low, inner, axis=1),
            jnp.take_along_axis(high, inner, axis=1),
        )

    for g in range(groups):
        run_low = run_low + far_tile[g : g + 1]
        run_high = run_high + far_tile[4 + g : 5 + g]
        order = (integ * (groups * me + g + 1)).astype(F32)
        low = jnp.broadcast_to(order * far_tile[2:3] / run_low, (SUB, LANES))
        high = jnp.broadcast_to(order * far_tile[6:7] / run_high, (SUB, LANES))
        for r0 in range(0, rows, SUB):
            span = pl.ds(r0, SUB)
            factor[g, span] = gain[span] * looked_up(bins[span], low, high)
        factor[g, pl.ds(rows, SUB)] = halo_gain[...] * looked_up(halo_bins[...], low, high)
    for shift in (0, 1):
        block = jnp.concatenate([factor[g, pl.ds(shift, rows)] for g in range(groups)], axis=0)
        block = jnp.transpose(block)
        if shift:
            block = block * ones_past
        factor_rows[pl.ds(shift * LANES, LANES)] = block
    reach_rows = 2 * LANES - SUB
    for t in range(integ):
        norm[t, pl.ds(0, LANES)] = norm[t, pl.ds(0, LANES)] * factor_rows[pl.ds(0, LANES)] - 1.0
        span = pl.ds(LANES, reach_rows - LANES)
        norm[t, span] = norm[t, span] * factor_rows[span] - ones_past

    def score_copy(i, dst):
        return remote(
            scores.at[i],
            out_ref.at[pl.ds(groups * me, groups)],
            score_send.at[i],
            score_recv.at[i],
            {"section": dst},
        )

    def target(i):
        m, r = i // 2, i % 2
        return (me + ns // 2 + m - r * (2 * m + 1)) % ns

    def one_stride(i, carry):
        dst = target(i)
        k = dst + 1
        first_group = lane < rows

        def by_group(values):
            return jnp.where(first_group, values[0], values[1])

        levels = [
            by_group([cut[g, dst, d].astype(F32) * (4.0 / 256.0) for g in range(groups)])
            for d in range(integ)
        ]
        weight = by_group(
            [jnp.where(k <= reach[groups * me + g], 0.25 / integ, 0.0) for g in range(groups)]
        )

        chunk = 4

        def lower(b, inner):
            for c in range(chunk):
                r = pl.multiple_of((b * chunk + c) * SUB, SUB)
                for q in range(integ // 4):

                    def x(t, n):
                        return norm[4 * q + t, pl.ds(r + n * k, SUB)]

                    x0, x10, x11 = x(0, 0), x(1, 0), x(1, 1)
                    x20, x21, x22 = x(2, 0), x(2, 1), x(2, 2)
                    x30, x31, x32, x33 = x(3, 0), x(3, 1), x(3, 2), x(3, 3)
                    u0, u1 = x0 + x10, x0 + x11
                    span = pl.ds(r, SUB)
                    quads[4 * q, span] = u0 + (x20 + x30)
                    quads[4 * q + 1, span] = u0 + (x21 + x31)
                    quads[4 * q + 2, span] = u1 + (x21 + x32)
                    quads[4 * q + 3, span] = u1 + (x22 + x33)
            return inner

        tall = chunk * SUB
        lax.fori_loop(0, (LANES + 12 * k + tall - 1) // tall, lower, 0)

        def upper(b, inner):
            for c in range(chunk):
                r = pl.multiple_of((b * chunk + c) * SUB, SUB)

                def y(row, n):
                    return quads[row, pl.ds(r + n * k, SUB)]

                sums_over = jnp.zeros((SUB, wide), F32)
                for a in range(integ // 4):
                    own = y(a, 0)
                    for h in (2 * a, 2 * a + 1):
                        e = h - a
                        first = own + y(4 + a, e)
                        for d in (2 * h, 2 * h + 1):
                            n = d - h
                            drift = first + (y(8 + a, n) + y(12 + a, n + e))
                            sums_over = sums_over + jnp.maximum(drift - levels[d], 0.0)
                total[pl.ds(r, SUB)] = sums_over * weight
            return inner

        lax.fori_loop(0, LANES // tall, upper, 0)
        turned = jnp.transpose(total[...])
        for g in range(groups):
            scores[i, g] = turned[g * rows : (g + 1) * rows]

        @pl.when(i < ns - 1)
        def _():
            score_copy(i, dst).start()

        return carry

    lax.fori_loop(0, ns, one_stride, 0)
    kept = pltpu.make_async_copy(
        scores.at[ns - 1], out_ref.at[pl.ds(groups * me, groups)], load_sem.at[0]
    )
    kept.start()
    for i in range(ns - 1):
        score_copy(i, target(i)).wait_recv()
    kept.wait()
    for c in near_copies + halo_copies + far_copies + early_copies:
        c.wait_send()
    for i in range(ns - 1):
        score_copy(i, target(i)).wait_send()


def shards(near_count, spectra, channel_gain, bandpass_bin, drift_range, hit_cutoff):
    groups, integ, chans = spectra.shape
    ns, nf = lax.axis_size("section"), lax.axis_size("freq")
    total_bins = 2 * LANES
    nc, nz = near_count, nf // near_count
    rows = chans // LANES
    wide = groups * rows
    sizes = (ns, nf, nc, groups, integ, chans, total_bins)
    dma = pltpu.SemaphoreType.DMA
    tile = (SUB, LANES)
    out = pl.pallas_call(
        functools.partial(kernel, sizes),
        out_shape=jax.ShapeDtypeStruct((ns * groups, rows, LANES), F32),
        in_specs=[pl.BlockSpec(memory_space=pltpu.HBM)] * 5,
        out_specs=pl.BlockSpec(memory_space=pl.ANY),
        scratch_shapes=[
            pltpu.VMEM((groups, integ, rows + SUB, LANES), F32),
            pltpu.VMEM((rows, LANES), F32),
            pltpu.VMEM((rows, LANES), jnp.int32),
            pltpu.SMEM((ns * groups,), jnp.int32),
            pltpu.SMEM((groups, *hit_cutoff.shape[1:]), jnp.int32),
            pltpu.VMEM((groups, integ, LANES), F32),
            pltpu.VMEM(tile, F32),
            pltpu.VMEM(tile, jnp.int32),
            pltpu.VMEM((groups, rows + SUB, LANES), F32),
            pltpu.VMEM((2 * LANES, wide), F32),
            pltpu.VMEM((integ, 2 * LANES, wide), F32),
            pltpu.VMEM((integ, 2 * LANES, wide), F32),
            pltpu.VMEM((LANES, wide), F32),
            pltpu.VMEM((ns, groups, rows, LANES), F32),
            pltpu.VMEM(tile, F32),
            pltpu.VMEM((max(nc - 1, 1), *tile), F32),
            pltpu.VMEM(tile, F32),
            pltpu.VMEM((max(nz - 1, 1), *tile), F32),
            pltpu.VMEM(tile, F32),
            pltpu.VMEM((ns - 1, *tile), F32),
            dma((groups * integ,)),
            dma((4,)),
            dma((max(nc - 1, 1),)),
            dma((max(nc - 1, 1),)),
            dma((max(nz - 1, 1),)),
            dma((max(nz - 1, 1),)),
            dma((ns - 1,)),
            dma((ns - 1,)),
            dma((3,)),
            dma((3,)),
            dma((ns - 1,)),
            dma((ns - 1,)),
        ],
        compiler_params=pltpu.CompilerParams(
            collective_id=0, has_side_effects=True, vmem_limit_bytes=16 << 20
        ),
    )(*[pltpu.with_memory_space_constraint(v, pltpu.HBM) for v in (
        spectra.reshape(groups, integ // SUB, SUB, rows, LANES).transpose(0, 1, 3, 2, 4),
        channel_gain.reshape(rows, LANES),
        bandpass_bin.reshape(rows, LANES),
        drift_range,
        hit_cutoff,
    )])
    return out.reshape(ns * groups, 1, chans)


def solution(mesh, near_count=8):
    return jax.shard_map(
        functools.partial(shards, near_count),
        mesh=mesh,
        in_specs=(P("section", None, "freq"), P("freq"), P("freq"), P(), P()),
        out_specs=P(None, "section", "freq"),
        check_vma=False,
    )
```

```python
import functools

import jax
import jax.numpy as jnp
from jax import lax
from jax.experimental import pallas as pl
from jax.experimental.pallas import tpu as pltpu
from jax.sharding import PartitionSpec as P

F32 = jnp.float32
BF16 = jnp.bfloat16
LANES = 128
SUB = 8
MESH = pl.DeviceIdType.MESH


def remote(src, dst, send, recv, where):
    return pltpu.make_async_remote_copy(
        src_ref=src, dst_ref=dst, send_sem=send, recv_sem=recv, device_id=where, device_id_type=MESH
    )


def kernel(
    sizes,
    spec_hbm,
    gain_hbm,
    bins_hbm,
    reach_hbm,
    cut_hbm,
    out_ref,
    nat,
    gain,
    bins,
    reach,
    cut,
    halo,
    halo_gain,
    halo_bins,
    factor,
    factor_rows,
    norm,
    quads,
    total,
    scores,
    part,
    near,
    near_sum,
    far,
    far_sum,
    early,
    spec_sem,
    load_sem,
    near_send,
    near_recv,
    far_send,
    far_recv,
    early_send,
    early_recv,
    halo_send,
    halo_recv,
    score_send,
    score_recv,
):
    ns, nf, nc, groups, integ, chans, total_bins = sizes
    nz = nf // nc
    rows = chans // LANES
    wide = groups * rows
    me = lax.axis_index("section")
    here = lax.axis_index("freq")
    z, xc = lax.div(here, nc), lax.rem(here, nc)

    at_end = here == nf - 1
    near_peers = [z * nc + lax.rem(xc + d, nc) for d in range(1, nc)]
    far_peers = [lax.rem(here + d * nc, nf) for d in range(1, nz)]
    section_peers = [lax.rem(me + d, ns) for d in range(1, ns)]
    left, right = lax.rem(here + nf - 1, nf), lax.rem(here + 1, nf)

    loads = [
        pltpu.make_async_copy(bins_hbm, bins, load_sem.at[0]),
        pltpu.make_async_copy(gain_hbm, gain, load_sem.at[1]),
        pltpu.make_async_copy(reach_hbm, reach, load_sem.at[2]),
        pltpu.make_async_copy(cut_hbm.at[pl.ds(groups * me, groups)], cut, load_sem.at[3]),
    ]
    spec_loads = [
        pltpu.make_async_copy(
            spec_hbm.at[g, t // SUB, :, t % SUB, :],
            nat.at[g, t, pl.ds(0, rows)],
            spec_sem.at[g * integ + t],
        )
        for g in range(groups)
        for t in range(integ)
    ]
    for c in loads[:2] + spec_loads:
        c.start()

    barrier = pltpu.get_barrier_semaphore()
    for peer in section_peers:
        pl.semaphore_signal(barrier, inc=1, device_id={"section": peer}, device_id_type=MESH)
    for peer in far_peers + [left, right] + near_peers:
        pl.semaphore_signal(barrier, inc=1, device_id={"freq": peer}, device_id_type=MESH)

    for c in loads[2:]:
        c.start()
    for c in loads[:2]:
        c.wait()
    bin_row = lax.broadcasted_iota(jnp.int32, (total_bins, LANES), 0).astype(F32).astype(BF16)
    named = bins[...].astype(F32).astype(BF16)
    for c in spec_loads:
        c.wait()
    acc = jnp.zeros((SUB, total_bins), F32)
    for r0 in range(0, rows, SUB):
        span = pl.ds(r0, SUB)
        high, middle, low = [], [], []
        for g in range(groups):
            value = nat[g, 0, span]
            for t in range(1, integ):
                value = value + nat[g, t, span]
            value = value * gain[span]
            high.append(value.astype(BF16).astype(F32))
            value = value - high[-1]
            middle.append(value.astype(BF16).astype(F32))
            low.append(value - middle[-1])
        ones = [jnp.ones((SUB, LANES), F32)] * 2
        turned = jnp.transpose(jnp.stack(high + middle + low + ones), (1, 0, 2))
        lhs = jnp.concatenate([turned[r] for r in range(SUB)], axis=1).astype(BF16)
        one_hot = jnp.concatenate(
            [
                jnp.where(bin_row == named[r : r + 1], jnp.ones((), BF16), jnp.zeros((), BF16))
                for r in range(r0, r0 + SUB)
            ],
            axis=1,
        )
        acc = acc + lax.dot_general(
            lhs,
            one_hot,
            (((1,), (1,)), ((), ())),
            preferred_element_type=F32,
        )
    sums = acc[0:2] + acc[2:4] + acc[4:6]
    counts = acc[6:8]
    tile = jnp.concatenate(
        [sums[:, :LANES], counts[:1, :LANES], sums[:, LANES:], counts[:1, LANES:]], axis=0
    )
    part[...] = tile

    pl.semaphore_wait(barrier, nc + nz + ns - 1)

    near_copies = [
        remote(part, near.at[d], near_send.at[d], near_recv.at[d], {"freq": p})
        for d, p in enumerate(near_peers)
    ]
    halo_copies = [
        remote(src, dst, halo_send.at[i], halo_recv.at[i], {"freq": left})
        for i, (src, dst) in enumerate(
            [
                (nat.at[:, :, 0], halo),
                (gain.at[pl.ds(0, SUB)], halo_gain),
                (bins.at[pl.ds(0, SUB)], halo_bins),
            ]
        )
    ]
    for c in near_copies + halo_copies:
        c.start()

    def turn(t, shift):
        block = jnp.concatenate(
            [nat[g, t, pl.ds(shift, rows)] for g in range(groups)], axis=0
        )
        norm[t, pl.ds(shift * LANES, LANES)] = jnp.transpose(block)

    for t in range(integ):
        turn(t, 0)
    for c in near_copies:
        c.wait_recv()
    near_tile = tile
    for d in range(nc - 1):
        near_tile = near_tile + near[d]
    near_sum[...] = near_tile
    far_copies = [
        remote(near_sum, far.at[d], far_send.at[d], far_recv.at[d], {"freq": p})
        for d, p in enumerate(far_peers)
    ]
    for c in far_copies:
        c.start()

    for c in halo_copies:
        c.wait_recv()
    for g in range(groups):
        for t in range(integ):
            nat[g, t, pl.ds(rows, 1)] = jnp.where(at_end, 1.0, halo[g, t : t + 1])
    for t in range(integ):
        turn(t, 1)

    for c in far_copies:
        c.wait_recv()
    far_tile = near_tile
    for d in range(nz - 1):
        far_tile = far_tile + far[d]
    far_sum[...] = jnp.concatenate(
        [far_tile[0:1] + far_tile[1:2], far_tile[3:4] + far_tile[4:5]], axis=0
    )
    early_copies = [
        remote(far_sum, early.at[d], early_send.at[d], early_recv.at[d], {"section": p})
        for d, p in enumerate(section_peers)
    ]
    for c in early_copies:
        c.start()

    for c in loads[2:]:
        c.wait()
    lane = lax.broadcasted_iota(jnp.int32, (SUB, wide), 1)
    for c in early_copies:
        c.wait_recv()
    before = jnp.zeros((2, LANES), F32)
    for d in range(1, ns):
        before = before + jnp.where(d <= me, early[d - 1], 0.0)
    run_low, run_high = before[0:1], before[1:2]

    def looked_up(at, low, high):
        inner = jnp.bitwise_and(at, LANES - 1)
        return jnp.where(
            at < LANES,
            jnp.take_along_axis(low, inner, axis=1),
            jnp.take_along_axis(high, inner, axis=1),
        )

    for g in range(groups):
        run_low = run_low + far_tile[g : g + 1]
        run_high = run_high + far_tile[3 + g : 4 + g]
        order = (integ * (groups * me + g + 1)).astype(F32)
        low = jnp.broadcast_to(order * far_tile[2:3] / run_low, (SUB, LANES))
        high = jnp.broadcast_to(order * far_tile[5:6] / run_high, (SUB, LANES))
        for r0 in range(0, rows, SUB):
            span = pl.ds(r0, SUB)
            factor[g, span] = gain[span] * looked_up(bins[span], low, high)
        past = halo_gain[...] * looked_up(halo_bins[...], low, high)
        factor[g, pl.ds(rows, SUB)] = jnp.where(at_end, 1.0, past)
    for shift in (0, 1):
        block = jnp.concatenate([factor[g, pl.ds(shift, rows)] for g in range(groups)], axis=0)
        factor_rows[pl.ds(shift * LANES, LANES)] = jnp.transpose(block)

    def score_copy(i, dst):
        return remote(
            scores.at[i],
            out_ref.at[pl.ds(groups * me, groups)],
            score_send.at[i],
            score_recv.at[i],
            {"section": dst},
        )

    def target(i):
        m, r = i // 2, i % 2
        return lax.rem(me + ns // 2 + m - r * (2 * m + 1), ns)

    def one_stride(i, carry):
        dst = target(i)
        k = dst + 1
        first_group = lane < rows

        def by_group(values):
            return jnp.where(first_group, values[0], values[1])

        levels = [
            by_group([cut[g, dst, d].astype(F32) * (4.0 / 256.0) + integ for g in range(groups)])
            for d in range(integ)
        ]
        weight = by_group(
            [jnp.where(k <= reach[groups * me + g], 0.25 / integ, 0.0) for g in range(groups)]
        )

        chunk = 4

        def lower(b, inner):
            for c in range(chunk):
                r = pl.multiple_of((b * chunk + c) * SUB, SUB)
                scale = [factor_rows[pl.ds(r + n * k, SUB)] for n in range(4)]
                for q in range(integ // 4):

                    def x(t, n):
                        return norm[4 * q + t, pl.ds(r + n * k, SUB)] * scale[n]

                    x0, x10, x11 = x(0, 0), x(1, 0), x(1, 1)
                    x20, x21, x22 = x(2, 0), x(2, 1), x(2, 2)
                    x30, x31, x32, x33 = x(3, 0), x(3, 1), x(3, 2), x(3, 3)
                    u0, u1 = x0 + x10, x0 + x11
                    span = pl.ds(r, SUB)
                    quads[4 * q, span] = u0 + (x20 + x30)
                    quads[4 * q + 1, span] = u0 + (x21 + x31)
                    quads[4 * q + 2, span] = u1 + (x21 + x32)
                    quads[4 * q + 3, span] = u1 + (x22 + x33)
            return inner

        tall = chunk * SUB
        lax.fori_loop(0, (LANES + 12 * k + tall - 1) // tall, lower, 0)

        def upper(b, inner):
            for c in range(chunk):
                r = pl.multiple_of((b * chunk + c) * SUB, SUB)

                def y(row, n):
                    return quads[row, pl.ds(r + n * k, SUB)]

                sums_over = jnp.zeros((SUB, wide), F32)
                for a in range(integ // 4):
                    own = y(a, 0)
                    for h in (2 * a, 2 * a + 1):
                        e = h - a
                        first = own + y(4 + a, e)
                        for d in (2 * h, 2 * h + 1):
                            n = d - h
                            drift = first + (y(8 + a, n) + y(12 + a, n + e))
                            sums_over = sums_over + jnp.maximum(drift - levels[d], 0.0)
                total[pl.ds(r, SUB)] = sums_over * weight
            return inner

        lax.fori_loop(0, LANES // tall, upper, 0)
        turned = jnp.transpose(total[...])
        for g in range(groups):
            scores[i, g] = turned[g * rows : (g + 1) * rows]

        @pl.when(i < ns - 1)
        def _():
            score_copy(i, dst).start()

        return carry

    lax.fori_loop(0, ns, one_stride, 0)
    kept = pltpu.make_async_copy(
        scores.at[ns - 1], out_ref.at[pl.ds(groups * me, groups)], load_sem.at[0]
    )
    kept.start()
    for c in near_copies + halo_copies + far_copies + early_copies:
        c.wait_send()
    for i in range(ns - 1):
        score_copy(i, target(i)).wait_recv()
    kept.wait()
    for i in range(ns - 1):
        score_copy(i, target(i)).wait_send()


def shards(near_count, spectra, channel_gain, bandpass_bin, drift_range, hit_cutoff):
    groups, integ, chans = spectra.shape
    ns, nf = lax.axis_size("section"), lax.axis_size("freq")
    total_bins = 2 * LANES
    nc, nz = near_count, nf // near_count
    rows = chans // LANES
    wide = groups * rows
    sizes = (ns, nf, nc, groups, integ, chans, total_bins)
    dma = pltpu.SemaphoreType.DMA
    tile = (SUB, LANES)
    out = pl.pallas_call(
        functools.partial(kernel, sizes),
        out_shape=jax.ShapeDtypeStruct((ns * groups, rows, LANES), F32),
        in_specs=[pl.BlockSpec(memory_space=pltpu.HBM)] * 5,
        out_specs=pl.BlockSpec(memory_space=pl.ANY),
        scratch_shapes=[
            pltpu.VMEM((groups, integ, rows + SUB, LANES), F32),
            pltpu.VMEM((rows, LANES), F32),
            pltpu.VMEM((rows, LANES), jnp.int32),
            pltpu.SMEM((ns * groups,), jnp.int32),
            pltpu.SMEM((groups, *hit_cutoff.shape[1:]), jnp.int32),
            pltpu.VMEM((groups, integ, LANES), F32),
            pltpu.VMEM(tile, F32),
            pltpu.VMEM(tile, jnp.int32),
            pltpu.VMEM((groups, rows + SUB, LANES), F32),
            pltpu.VMEM((2 * LANES, wide), F32),
            pltpu.VMEM((integ, 2 * LANES + SUB, wide), F32),
            pltpu.VMEM((integ, 2 * LANES + SUB, wide), F32),
            pltpu.VMEM((LANES, wide), F32),
            pltpu.VMEM((ns, groups, rows, LANES), F32),
            pltpu.VMEM((6, LANES), F32),
            pltpu.VMEM((max(nc - 1, 1), 6, LANES), F32),
            pltpu.VMEM((6, LANES), F32),
            pltpu.VMEM((max(nz - 1, 1), 6, LANES), F32),
            pltpu.VMEM((2, LANES), F32),
            pltpu.VMEM((ns - 1, 2, LANES), F32),
            dma((groups * integ,)),
            dma((4,)),
            dma((max(nc - 1, 1),)),
            dma((max(nc - 1, 1),)),
            dma((max(nz - 1, 1),)),
            dma((max(nz - 1, 1),)),
            dma((ns - 1,)),
            dma((ns - 1,)),
            dma((3,)),
            dma((3,)),
            dma((ns - 1,)),
            dma((ns - 1,)),
        ],
        compiler_params=pltpu.CompilerParams(
            collective_id=0, has_side_effects=True, vmem_limit_bytes=16 << 20
        ),
    )(*[pltpu.with_memory_space_constraint(v, pltpu.HBM) for v in (
        spectra.reshape(groups, integ // SUB, SUB, rows, LANES).transpose(0, 1, 3, 2, 4),
        channel_gain.reshape(rows, LANES),
        bandpass_bin.reshape(rows, LANES),
        drift_range,
        hit_cutoff,
    )])
    return out.reshape(ns * groups, 1, chans)


def solution(mesh, near_count=8):
    return jax.shard_map(
        functools.partial(shards, near_count),
        mesh=mesh,
        in_specs=(P("section", None, "freq"), P("freq"), P("freq"), P(), P()),
        out_specs=P(None, "section", "freq"),
        check_vma=False,
    )
```

```python
import functools

import jax
import jax.numpy as jnp
from jax import lax
from jax.experimental import pallas as pl
from jax.experimental.pallas import tpu as pltpu
from jax.sharding import PartitionSpec as P

F32 = jnp.float32
BF16 = jnp.bfloat16
LANES = 128
SUB = 8
MESH = pl.DeviceIdType.MESH


def remote(src, dst, send, recv, where):
    return pltpu.make_async_remote_copy(
        src_ref=src, dst_ref=dst, send_sem=send, recv_sem=recv, device_id=where, device_id_type=MESH
    )


def kernel(
    sizes,
    spec_hbm,
    gain_hbm,
    bins_hbm,
    reach_hbm,
    cut_hbm,
    out_ref,
    nat,
    gain,
    bins,
    reach,
    cut,
    halo,
    halo_gain,
    halo_bins,
    factor,
    factor_rows,
    norm,
    quads,
    total,
    scores,
    part,
    near,
    near_sum,
    far,
    far_sum,
    early,
    before,
    far_ready,
    section_ready,
    spec_sem,
    load_sem,
    near_send,
    near_recv,
    far_send,
    far_recv,
    early_send,
    early_recv,
    halo_send,
    halo_recv,
    score_send,
    score_recv,
):
    ns, nf, nc, groups, integ, chans, total_bins = sizes
    nz = nf // nc
    rows = chans // LANES
    wide = groups * rows
    me = lax.axis_index("section")
    here = lax.axis_index("freq")
    z, xc = lax.div(here, nc), lax.rem(here, nc)

    at_end = here == nf - 1
    near_peers = [z * nc + lax.rem(xc + d, nc) for d in range(1, nc)]
    far_peers = [lax.rem(here + d * nc, nf) for d in range(1, nz)]
    section_peers = [lax.rem(me + d, ns) for d in range(1, ns)]
    left, right = lax.rem(here + nf - 1, nf), lax.rem(here + 1, nf)

    loads = [
        pltpu.make_async_copy(bins_hbm, bins, load_sem.at[0]),
        pltpu.make_async_copy(gain_hbm, gain, load_sem.at[1]),
        pltpu.make_async_copy(reach_hbm, reach, load_sem.at[2]),
        pltpu.make_async_copy(cut_hbm.at[pl.ds(groups * me, groups)], cut, load_sem.at[3]),
    ]
    spec_loads = [
        pltpu.make_async_copy(
            spec_hbm.at[g, t // SUB, :, t % SUB, :],
            nat.at[g, t, pl.ds(0, rows)],
            spec_sem.at[g * integ + t],
        )
        for g in range(groups)
        for t in range(integ)
    ]
    for c in loads[:2] + spec_loads:
        c.start()

    barrier = pltpu.get_barrier_semaphore()
    def greet(sem, cond, where):
        @pl.when(cond)
        def _():
            pl.semaphore_signal(sem, inc=1, device_id=where, device_id_type=MESH)

    for d, peer in enumerate(section_peers, 1):
        greet(barrier, me + d < ns, {"section": peer})
    for d, peer in enumerate(far_peers, 1):
        greet(barrier, z + d < nz, {"freq": peer})
    greet(barrier, here < nf - 1, {"freq": right})
    for peer in near_peers:
        pl.semaphore_signal(barrier, inc=1, device_id={"freq": peer}, device_id_type=MESH)

    for c in loads[2:]:
        c.start()
    for c in loads[:2]:
        c.wait()
    bin_row = lax.broadcasted_iota(jnp.int32, (total_bins, LANES), 0).astype(F32).astype(BF16)
    named = bins[...].astype(F32).astype(BF16)
    for c in spec_loads:
        c.wait()
    acc = jnp.zeros((SUB, total_bins), F32)
    for r0 in range(0, rows, SUB):
        span = pl.ds(r0, SUB)
        high, middle, low = [], [], []
        for g in range(groups):
            value = nat[g, 0, span]
            for t in range(1, integ):
                value = value + nat[g, t, span]
            value = value * gain[span]
            high.append(value.astype(BF16).astype(F32))
            value = value - high[-1]
            middle.append(value.astype(BF16).astype(F32))
            low.append(value - middle[-1])
        ones = [jnp.ones((SUB, LANES), F32)] * 2
        turned = jnp.transpose(jnp.stack(high + middle + low + ones), (1, 0, 2))
        lhs = jnp.concatenate([turned[r] for r in range(SUB)], axis=1).astype(BF16)
        one_hot = jnp.concatenate(
            [
                jnp.where(bin_row == named[r : r + 1], jnp.ones((), BF16), jnp.zeros((), BF16))
                for r in range(r0, r0 + SUB)
            ],
            axis=1,
        )
        acc = acc + lax.dot_general(
            lhs,
            one_hot,
            (((1,), (1,)), ((), ())),
            preferred_element_type=F32,
        )
    sums = acc[0:2] + acc[2:4] + acc[4:6]
    counts = acc[6:8]
    tile = jnp.concatenate(
        [sums[:, :LANES], counts[:1, :LANES], sums[:, LANES:], counts[:1, LANES:]], axis=0
    )
    part[...] = tile

    pl.semaphore_wait(barrier, nc - 1 + z + me + jnp.where(here > 0, 1, 0))
    for d, peer in enumerate(far_peers, 1):
        greet(far_ready, z + d >= nz, {"freq": peer})
    for d, peer in enumerate(section_peers, 1):
        greet(section_ready, me + d >= ns, {"section": peer})

    near_copies = [
        remote(part, near.at[d], near_send.at[d], near_recv.at[d], {"freq": p})
        for d, p in enumerate(near_peers)
    ]
    halo_copies = [
        remote(src, dst, halo_send.at[i], halo_recv.at[i], {"freq": left})
        for i, (src, dst) in enumerate(
            [
                (nat.at[:, :, 0], halo),
                (gain.at[pl.ds(0, SUB)], halo_gain),
                (bins.at[pl.ds(0, SUB)], halo_bins),
            ]
        )
    ]
    for c in near_copies:
        c.start()

    @pl.when(here > 0)
    def _():
        for c in halo_copies:
            c.start()

    def turn(t, shift):
        block = jnp.concatenate(
            [nat[g, t, pl.ds(shift, rows)] for g in range(groups)], axis=0
        )
        norm[t, pl.ds(shift * LANES, LANES)] = jnp.transpose(block)

    for t in range(integ):
        turn(t, 0)
    for c in near_copies:
        c.wait_recv()
    near_tile = tile
    for d in range(nc - 1):
        near_tile = near_tile + near[d]
    near_sum[...] = near_tile
    far_copies = [
        remote(near_sum, far.at[d], far_send.at[d], far_recv.at[d], {"freq": p})
        for d, p in enumerate(far_peers)
    ]
    for d, c in enumerate(far_copies, 1):
        pl.when(z + d >= nz)(c.start)

    @pl.when(here < nf - 1)
    def _():
        for c in halo_copies:
            c.wait_recv()

    for g in range(groups):
        for t in range(integ):
            nat[g, t, pl.ds(rows, 1)] = jnp.where(at_end, 1.0, halo[g, t : t + 1])
    for t in range(integ):
        turn(t, 1)

    @pl.when(z < nz - 1)
    def _():
        pl.semaphore_wait(far_ready, nz - 1 - z)

    for d, c in enumerate(far_copies, 1):
        pl.when(z + d < nz)(c.start)
    for c in far_copies:
        c.wait_recv()
    far_tile = near_tile
    for d in range(nz - 1):
        far_tile = far_tile + far[d]
    far_sum[...] = jnp.concatenate(
        [far_tile[0:1] + far_tile[1:2], far_tile[3:4] + far_tile[4:5]], axis=0
    )
    early_copies = [
        remote(far_sum, early.at[d], early_send.at[d], early_recv.at[d], {"section": p})
        for d, p in enumerate(section_peers)
    ]
    @pl.when(me < ns - 1)
    def _():
        pl.semaphore_wait(section_ready, ns - 1 - me)

    for d, c in enumerate(early_copies, 1):
        pl.when(me + d < ns)(c.start)
    before[...] = jnp.zeros((2, LANES), F32)

    for c in loads[2:]:
        c.wait()
    lane = lax.broadcasted_iota(jnp.int32, (SUB, wide), 1)
    for d, c in enumerate(early_copies, 1):

        @pl.when(d <= me)
        def _():
            c.wait_recv()
            before[...] += early[d - 1]

    run_low, run_high = before[0:1], before[1:2]

    def looked_up(at, low, high):
        inner = jnp.bitwise_and(at, LANES - 1)
        return jnp.where(
            at < LANES,
            jnp.take_along_axis(low, inner, axis=1),
            jnp.take_along_axis(high, inner, axis=1),
        )

    for g in range(groups):
        run_low = run_low + far_tile[g : g + 1]
        run_high = run_high + far_tile[3 + g : 4 + g]
        order = (integ * (groups * me + g + 1)).astype(F32)
        low = jnp.broadcast_to(order * far_tile[2:3] / run_low, (SUB, LANES))
        high = jnp.broadcast_to(order * far_tile[5:6] / run_high, (SUB, LANES))
        for r0 in range(0, rows, SUB):
            span = pl.ds(r0, SUB)
            factor[g, span] = gain[span] * looked_up(bins[span], low, high)
        past = halo_gain[...] * looked_up(halo_bins[...], low, high)
        factor[g, pl.ds(rows, SUB)] = jnp.where(at_end, 1.0, past)
    for shift in (0, 1):
        block = jnp.concatenate([factor[g, pl.ds(shift, rows)] for g in range(groups)], axis=0)
        factor_rows[pl.ds(shift * LANES, LANES)] = jnp.transpose(block)

    def score_copy(i, off):
        return remote(
            scores.at[i],
            out_ref.at[pl.ds(groups * me, groups)],
            score_send.at[i],
            score_recv.at[off - 1],
            {"section": lax.rem(me + off, ns)},
        )

    def plain(i):
        m, r = lax.div(i, 2), lax.rem(i, 2)
        return ns // 2 + m - r * (2 * m + 1)

    top = lax.rem(ns - me, ns)
    place = jnp.where(top >= ns // 2, 2 * top - ns, ns - 1 - 2 * top)

    def offset(i):
        moved = jnp.where(i == 0, top, plain(jnp.where(i <= place, i - 1, i)))
        return jnp.where(me == 0, plain(i), moved)

    def one_stride(i, carry):
        off = offset(i)
        dst = lax.rem(me + off, ns)
        k = dst + 1
        first_group = lane < rows

        def by_group(values):
            return jnp.where(first_group, values[0], values[1])

        levels = [
            by_group([cut[g, dst, d].astype(F32) * (4.0 / 256.0) + integ for g in range(groups)])
            for d in range(integ)
        ]
        weight = by_group(
            [jnp.where(k <= reach[groups * me + g], 0.25 / integ, 0.0) for g in range(groups)]
        )

        chunk = 4

        def lower(b, inner):
            for c in range(chunk):
                r = pl.multiple_of((b * chunk + c) * SUB, SUB)
                scale = [factor_rows[pl.ds(r + n * k, SUB)] for n in range(4)]
                for q in range(integ // 4):

                    def x(t, n):
                        return norm[4 * q + t, pl.ds(r + n * k, SUB)] * scale[n]

                    x0, x10, x11 = x(0, 0), x(1, 0), x(1, 1)
                    x20, x21, x22 = x(2, 0), x(2, 1), x(2, 2)
                    x30, x31, x32, x33 = x(3, 0), x(3, 1), x(3, 2), x(3, 3)
                    u0, u1 = x0 + x10, x0 + x11
                    span = pl.ds(r, SUB)
                    quads[4 * q, span] = u0 + (x20 + x30)
                    quads[4 * q + 1, span] = u0 + (x21 + x31)
                    quads[4 * q + 2, span] = u1 + (x21 + x32)
                    quads[4 * q + 3, span] = u1 + (x22 + x33)
            return inner

        tall = chunk * SUB
        lax.fori_loop(0, (LANES + 12 * k + tall - 1) // tall, lower, 0)

        def upper(b, inner):
            for c in range(chunk):
                r = pl.multiple_of((b * chunk + c) * SUB, SUB)

                def y(row, n):
                    return quads[row, pl.ds(r + n * k, SUB)]

                sums_over = jnp.zeros((SUB, wide), F32)
                for a in range(integ // 4):
                    own = y(a, 0)
                    for h in (2 * a, 2 * a + 1):
                        e = h - a
                        first = own + y(4 + a, e)
                        for d in (2 * h, 2 * h + 1):
                            n = d - h
                            drift = first + (y(8 + a, n) + y(12 + a, n + e))
                            sums_over = sums_over + jnp.maximum(drift - levels[d], 0.0)
                total[pl.ds(r, SUB)] = sums_over * weight
            return inner

        lax.fori_loop(0, LANES // tall, upper, 0)
        turned = jnp.transpose(total[...])
        for g in range(groups):
            scores[i, g] = turned[g * rows : (g + 1) * rows]

        @pl.when(i < ns - 1)
        def _():
            score_copy(i, off).start()

        return carry

    lax.fori_loop(0, ns, one_stride, 0)
    kept = pltpu.make_async_copy(
        scores.at[ns - 1], out_ref.at[pl.ds(groups * me, groups)], load_sem.at[0]
    )
    kept.start()
    for c in near_copies + far_copies:
        c.wait_send()

    @pl.when(here > 0)
    def _():
        for c in halo_copies:
            c.wait_send()

    for d, c in enumerate(early_copies, 1):
        pl.when(me + d < ns)(c.wait_send)
    for i in range(ns - 1):
        score_copy(i, i + 1).wait_recv()
    kept.wait()
    for i in range(ns - 1):
        score_copy(i, i + 1).wait_send()


def shards(near_count, spectra, channel_gain, bandpass_bin, drift_range, hit_cutoff):
    groups, integ, chans = spectra.shape
    ns, nf = lax.axis_size("section"), lax.axis_size("freq")
    total_bins = 2 * LANES
    nc, nz = near_count, nf // near_count
    rows = chans // LANES
    wide = groups * rows
    sizes = (ns, nf, nc, groups, integ, chans, total_bins)
    dma = pltpu.SemaphoreType.DMA
    tile = (SUB, LANES)
    out = pl.pallas_call(
        functools.partial(kernel, sizes),
        out_shape=jax.ShapeDtypeStruct((ns * groups, rows, LANES), F32),
        in_specs=[pl.BlockSpec(memory_space=pltpu.HBM)] * 5,
        out_specs=pl.BlockSpec(memory_space=pl.ANY),
        scratch_shapes=[
            pltpu.VMEM((groups, integ, rows + SUB, LANES), F32),
            pltpu.VMEM((rows, LANES), F32),
            pltpu.VMEM((rows, LANES), jnp.int32),
            pltpu.SMEM((ns * groups,), jnp.int32),
            pltpu.SMEM((groups, *hit_cutoff.shape[1:]), jnp.int32),
            pltpu.VMEM((groups, integ, LANES), F32),
            pltpu.VMEM(tile, F32),
            pltpu.VMEM(tile, jnp.int32),
            pltpu.VMEM((groups, rows + SUB, LANES), F32),
            pltpu.VMEM((2 * LANES, wide), F32),
            pltpu.VMEM((integ, 2 * LANES + SUB, wide), F32),
            pltpu.VMEM((integ, 2 * LANES + SUB, wide), F32),
            pltpu.VMEM((LANES, wide), F32),
            pltpu.VMEM((ns, groups, rows, LANES), F32),
            pltpu.VMEM((6, LANES), F32),
            pltpu.VMEM((max(nc - 1, 1), 6, LANES), F32),
            pltpu.VMEM((6, LANES), F32),
            pltpu.VMEM((max(nz - 1, 1), 6, LANES), F32),
            pltpu.VMEM((2, LANES), F32),
            pltpu.VMEM((ns - 1, 2, LANES), F32),
            pltpu.VMEM((2, LANES), F32),
            pltpu.SemaphoreType.REGULAR,
            pltpu.SemaphoreType.REGULAR,
            dma((groups * integ,)),
            dma((4,)),
            dma((max(nc - 1, 1),)),
            dma((max(nc - 1, 1),)),
            dma((max(nz - 1, 1),)),
            dma((max(nz - 1, 1),)),
            dma((ns - 1,)),
            dma((ns - 1,)),
            dma((3,)),
            dma((3,)),
            dma((ns - 1,)),
            dma((ns - 1,)),
        ],
        compiler_params=pltpu.CompilerParams(
            collective_id=0, has_side_effects=True, vmem_limit_bytes=16 << 20
        ),
    )(*[pltpu.with_memory_space_constraint(v, pltpu.HBM) for v in (
        spectra.reshape(groups, integ // SUB, SUB, rows, LANES).transpose(0, 1, 3, 2, 4),
        channel_gain.reshape(rows, LANES),
        bandpass_bin.reshape(rows, LANES),
        drift_range,
        hit_cutoff,
    )])
    return out.reshape(ns * groups, 1, chans)


def solution(mesh, near_count=8):
    return jax.shard_map(
        functools.partial(shards, near_count),
        mesh=mesh,
        in_specs=(P("section", None, "freq"), P("freq"), P("freq"), P(), P()),
        out_specs=P(None, "section", "freq"),
        check_vma=False,
    )
```

```python
import functools

import jax
import jax.numpy as jnp
from jax import lax
from jax.experimental import pallas as pl
from jax.experimental.pallas import tpu as pltpu
from jax.sharding import PartitionSpec as P

F32 = jnp.float32
BF16 = jnp.bfloat16
LANES = 128
SUB = 8
MESH = pl.DeviceIdType.MESH


def remote(src, dst, send, recv, where):
    return pltpu.make_async_remote_copy(
        src_ref=src, dst_ref=dst, send_sem=send, recv_sem=recv, device_id=where, device_id_type=MESH
    )


def kernel(
    sizes,
    spec_hbm,
    gain_hbm,
    bins_hbm,
    reach_hbm,
    cut_hbm,
    out_ref,
    nat,
    gain,
    bins,
    reach,
    cut,
    halo,
    halo_gain,
    halo_bins,
    factor,
    factor_rows,
    norm,
    quads,
    total,
    scores,
    part,
    near,
    near_sum,
    far,
    far_sum,
    early,
    before,
    far_ready,
    section_ready,
    spec_sem,
    load_sem,
    near_send,
    near_recv,
    far_send,
    far_recv,
    early_send,
    early_recv,
    halo_send,
    halo_recv,
    score_send,
    score_recv,
):
    ns, nf, nc, groups, integ, chans, total_bins = sizes
    nz = nf // nc
    rows = chans // LANES
    wide = groups * rows
    me = lax.axis_index("section")
    here = lax.axis_index("freq")
    z, xc = lax.div(here, nc), lax.rem(here, nc)

    at_end = here == nf - 1
    near_peers = [z * nc + lax.rem(xc + d, nc) for d in range(1, nc)]
    far_peers = [lax.rem(here + d * nc, nf) for d in range(1, nz)]
    section_peers = [lax.rem(me + d, ns) for d in range(1, ns)]
    left, right = lax.rem(here + nf - 1, nf), lax.rem(here + 1, nf)

    loads = [
        pltpu.make_async_copy(bins_hbm, bins, load_sem.at[0]),
        pltpu.make_async_copy(gain_hbm, gain, load_sem.at[1]),
        pltpu.make_async_copy(reach_hbm, reach, load_sem.at[2]),
        pltpu.make_async_copy(cut_hbm.at[pl.ds(groups * me, groups)], cut, load_sem.at[3]),
    ]
    spec_loads = [
        pltpu.make_async_copy(
            spec_hbm.at[g, t // SUB, :, t % SUB, :],
            nat.at[g, t, pl.ds(0, rows)],
            spec_sem.at[g * integ + t],
        )
        for g in range(groups)
        for t in range(integ)
    ]
    for c in loads[:2] + spec_loads:
        c.start()

    barrier = pltpu.get_barrier_semaphore()
    def greet(sem, cond, where):
        @pl.when(cond)
        def _():
            pl.semaphore_signal(sem, inc=1, device_id=where, device_id_type=MESH)

    for d, peer in enumerate(section_peers, 1):
        greet(barrier, me + d < ns, {"section": peer})
    for d, peer in enumerate(far_peers, 1):
        greet(barrier, z + d < nz, {"freq": peer})
    greet(barrier, here < nf - 1, {"freq": right})
    for peer in near_peers:
        pl.semaphore_signal(barrier, inc=1, device_id={"freq": peer}, device_id_type=MESH)

    for c in loads[2:]:
        c.start()
    for c in loads[:2]:
        c.wait()
    bin_row = lax.broadcasted_iota(jnp.int32, (total_bins, LANES), 0).astype(F32).astype(BF16)
    named = bins[...].astype(F32).astype(BF16)
    for c in spec_loads:
        c.wait()
    acc = jnp.zeros((SUB, total_bins), F32)
    for r0 in range(0, rows, SUB):
        span = pl.ds(r0, SUB)
        high, middle, low = [], [], []
        for g in range(groups):
            value = nat[g, 0, span]
            for t in range(1, integ):
                value = value + nat[g, t, span]
            value = value * gain[span]
            high.append(value.astype(BF16).astype(F32))
            value = value - high[-1]
            middle.append(value.astype(BF16).astype(F32))
            low.append(value - middle[-1])
        ones = [jnp.ones((SUB, LANES), F32)] * 2
        turned = jnp.transpose(jnp.stack(high + middle + low + ones), (1, 0, 2))
        lhs = jnp.concatenate([turned[r] for r in range(SUB)], axis=1).astype(BF16)
        one_hot = jnp.concatenate(
            [
                jnp.where(bin_row == named[r : r + 1], jnp.ones((), BF16), jnp.zeros((), BF16))
                for r in range(r0, r0 + SUB)
            ],
            axis=1,
        )
        acc = acc + lax.dot_general(
            lhs,
            one_hot,
            (((1,), (1,)), ((), ())),
            preferred_element_type=F32,
        )
    sums = acc[0:2] + acc[2:4] + acc[4:6]
    counts = acc[6:8]
    tile = jnp.concatenate(
        [sums[:, :LANES], counts[:1, :LANES], sums[:, LANES:], counts[:1, LANES:]], axis=0
    )
    part[...] = tile

    pl.semaphore_wait(barrier, nc - 1 + z + me + jnp.where(here > 0, 1, 0))
    for d, peer in enumerate(far_peers, 1):
        greet(far_ready, z + d >= nz, {"freq": peer})
    for d, peer in enumerate(section_peers, 1):
        greet(section_ready, me + d >= ns, {"section": peer})

    near_copies = [
        remote(part, near.at[d], near_send.at[d], near_recv.at[d], {"freq": p})
        for d, p in enumerate(near_peers)
    ]
    halo_copies = [
        remote(src, dst, halo_send.at[i], halo_recv.at[i], {"freq": left})
        for i, (src, dst) in enumerate(
            [
                (nat.at[:, :, 0], halo),
                (gain.at[pl.ds(0, SUB)], halo_gain),
                (bins.at[pl.ds(0, SUB)], halo_bins),
            ]
        )
    ]
    for c in near_copies:
        c.start()

    @pl.when(here > 0)
    def _():
        for c in halo_copies:
            c.start()

    def turn(t, shift):
        block = jnp.concatenate(
            [nat[g, t, pl.ds(shift, rows)] for g in range(groups)], axis=0
        )
        norm[t, pl.ds(shift * LANES, LANES)] = jnp.transpose(block)

    for t in range(integ):
        turn(t, 0)
    for c in near_copies:
        c.wait_recv()
    near_tile = tile
    for d in range(nc - 1):
        near_tile = near_tile + near[d]
    near_sum[...] = near_tile
    far_copies = [
        remote(near_sum, far.at[d], far_send.at[d], far_recv.at[d], {"freq": p})
        for d, p in enumerate(far_peers)
    ]
    for d, c in enumerate(far_copies, 1):
        pl.when(z + d >= nz)(c.start)

    @pl.when(here < nf - 1)
    def _():
        for c in halo_copies:
            c.wait_recv()

    for g in range(groups):
        for t in range(integ):
            nat[g, t, pl.ds(rows, 1)] = jnp.where(at_end, 1.0, halo[g, t : t + 1])
    for t in range(integ):
        turn(t, 1)

    @pl.when(z < nz - 1)
    def _():
        pl.semaphore_wait(far_ready, nz - 1 - z)

    for d, c in enumerate(far_copies, 1):
        pl.when(z + d < nz)(c.start)
    for c in far_copies:
        c.wait_recv()
    far_tile = near_tile
    for d in range(nz - 1):
        far_tile = far_tile + far[d]
    far_sum[...] = jnp.concatenate(
        [far_tile[0:1] + far_tile[1:2], far_tile[3:4] + far_tile[4:5]], axis=0
    )
    early_copies = [
        remote(far_sum, early.at[d], early_send.at[d], early_recv.at[d], {"section": p})
        for d, p in enumerate(section_peers)
    ]
    @pl.when(me < ns - 1)
    def _():
        pl.semaphore_wait(section_ready, ns - 1 - me)

    for d, c in enumerate(early_copies, 1):
        pl.when(me + d < ns)(c.start)
    before[...] = jnp.zeros((2, LANES), F32)

    for c in loads[2:]:
        c.wait()
    lane = lax.broadcasted_iota(jnp.int32, (SUB, wide), 1)
    for d, c in enumerate(early_copies, 1):

        @pl.when(d <= me)
        def _():
            c.wait_recv()
            before[...] += early[d - 1]

    run_low, run_high = before[0:1], before[1:2]

    def looked_up(at, low, high):
        inner = jnp.bitwise_and(at, LANES - 1)
        return jnp.where(
            at < LANES,
            jnp.take_along_axis(low, inner, axis=1),
            jnp.take_along_axis(high, inner, axis=1),
        )

    for g in range(groups):
        run_low = run_low + far_tile[g : g + 1]
        run_high = run_high + far_tile[3 + g : 4 + g]
        order = (integ * (groups * me + g + 1)).astype(F32)
        low = jnp.broadcast_to(order * far_tile[2:3] / run_low, (SUB, LANES))
        high = jnp.broadcast_to(order * far_tile[5:6] / run_high, (SUB, LANES))
        for r0 in range(0, rows, SUB):
            span = pl.ds(r0, SUB)
            factor[g, span] = gain[span] * looked_up(bins[span], low, high)
        past = halo_gain[...] * looked_up(halo_bins[...], low, high)
        factor[g, pl.ds(rows, SUB)] = jnp.where(at_end, 1.0, past)
    for shift in (0, 1):
        block = jnp.concatenate([factor[g, pl.ds(shift, rows)] for g in range(groups)], axis=0)
        factor_rows[pl.ds(shift * LANES, LANES)] = jnp.transpose(block)

    def score_copy(i, off):
        return remote(
            scores.at[i],
            out_ref.at[pl.ds(groups * me, groups)],
            score_send.at[i],
            score_recv.at[off - 1],
            {"section": lax.rem(me + off, ns)},
        )

    orders = [2042460, 469735, 351974, 1879269, 1893724, 1893675, 1894242, 2053345]
    order = orders[0]
    for section in range(1, ns):
        order = jnp.where(me == section, orders[section], order)

    def one_stride(i, order):
        off = lax.rem(order, ns)
        dst = lax.rem(me + off, ns)
        k = dst + 1
        first_group = lane < rows

        def by_group(values):
            return jnp.where(first_group, values[0], values[1])

        levels = [
            by_group([cut[g, dst, d].astype(F32) * (4.0 / 256.0) + integ for g in range(groups)])
            for d in range(integ)
        ]
        weight = by_group(
            [jnp.where(k <= reach[groups * me + g], 0.25 / integ, 0.0) for g in range(groups)]
        )

        chunk = 4

        def lower(b, inner):
            for c in range(chunk):
                r = pl.multiple_of((b * chunk + c) * SUB, SUB)
                scale = [factor_rows[pl.ds(r + n * k, SUB)] for n in range(4)]
                for q in range(integ // 4):

                    def x(t, n):
                        return norm[4 * q + t, pl.ds(r + n * k, SUB)] * scale[n]

                    x0, x10, x11 = x(0, 0), x(1, 0), x(1, 1)
                    x20, x21, x22 = x(2, 0), x(2, 1), x(2, 2)
                    x30, x31, x32, x33 = x(3, 0), x(3, 1), x(3, 2), x(3, 3)
                    u0, u1 = x0 + x10, x0 + x11
                    span = pl.ds(r, SUB)
                    quads[4 * q, span] = u0 + (x20 + x30)
                    quads[4 * q + 1, span] = u0 + (x21 + x31)
                    quads[4 * q + 2, span] = u1 + (x21 + x32)
                    quads[4 * q + 3, span] = u1 + (x22 + x33)
            return inner

        tall = chunk * SUB
        lax.fori_loop(0, (LANES + 12 * k + tall - 1) // tall, lower, 0)

        def upper(b, inner):
            for c in range(chunk):
                r = pl.multiple_of((b * chunk + c) * SUB, SUB)

                def y(row, n):
                    return quads[row, pl.ds(r + n * k, SUB)]

                sums_over = jnp.zeros((SUB, wide), F32)
                for a in range(integ // 4):
                    own = y(a, 0)
                    for h in (2 * a, 2 * a + 1):
                        e = h - a
                        first = own + y(4 + a, e)
                        for d in (2 * h, 2 * h + 1):
                            n = d - h
                            drift = first + (y(8 + a, n) + y(12 + a, n + e))
                            sums_over = sums_over + jnp.maximum(drift - levels[d], 0.0)
                total[pl.ds(r, SUB)] = sums_over * weight
            return inner

        lax.fori_loop(0, LANES // tall, upper, 0)
        turned = jnp.transpose(total[...])
        for g in range(groups):
            scores[i, g] = turned[g * rows : (g + 1) * rows]

        @pl.when(i < ns - 1)
        def _():
            score_copy(i, off).start()

        return lax.div(order, ns)

    lax.fori_loop(0, ns, one_stride, order)
    kept = pltpu.make_async_copy(
        scores.at[ns - 1], out_ref.at[pl.ds(groups * me, groups)], load_sem.at[0]
    )
    kept.start()
    for c in near_copies + far_copies:
        c.wait_send()

    @pl.when(here > 0)
    def _():
        for c in halo_copies:
            c.wait_send()

    for d, c in enumerate(early_copies, 1):
        pl.when(me + d < ns)(c.wait_send)
    for i in range(ns - 1):
        score_copy(i, i + 1).wait_recv()
    kept.wait()
    for i in range(ns - 1):
        score_copy(i, i + 1).wait_send()


def shards(near_count, spectra, channel_gain, bandpass_bin, drift_range, hit_cutoff):
    groups, integ, chans = spectra.shape
    ns, nf = lax.axis_size("section"), lax.axis_size("freq")
    total_bins = 2 * LANES
    nc, nz = near_count, nf // near_count
    rows = chans // LANES
    wide = groups * rows
    sizes = (ns, nf, nc, groups, integ, chans, total_bins)
    dma = pltpu.SemaphoreType.DMA
    tile = (SUB, LANES)
    out = pl.pallas_call(
        functools.partial(kernel, sizes),
        out_shape=jax.ShapeDtypeStruct((ns * groups, rows, LANES), F32),
        in_specs=[pl.BlockSpec(memory_space=pltpu.HBM)] * 5,
        out_specs=pl.BlockSpec(memory_space=pl.ANY),
        scratch_shapes=[
            pltpu.VMEM((groups, integ, rows + SUB, LANES), F32),
            pltpu.VMEM((rows, LANES), F32),
            pltpu.VMEM((rows, LANES), jnp.int32),
            pltpu.SMEM((ns * groups,), jnp.int32),
            pltpu.SMEM((groups, *hit_cutoff.shape[1:]), jnp.int32),
            pltpu.VMEM((groups, integ, LANES), F32),
            pltpu.VMEM(tile, F32),
            pltpu.VMEM(tile, jnp.int32),
            pltpu.VMEM((groups, rows + SUB, LANES), F32),
            pltpu.VMEM((2 * LANES, wide), F32),
            pltpu.VMEM((integ, 2 * LANES + SUB, wide), F32),
            pltpu.VMEM((integ, 2 * LANES + SUB, wide), F32),
            pltpu.VMEM((LANES, wide), F32),
            pltpu.VMEM((ns, groups, rows, LANES), F32),
            pltpu.VMEM((6, LANES), F32),
            pltpu.VMEM((max(nc - 1, 1), 6, LANES), F32),
            pltpu.VMEM((6, LANES), F32),
            pltpu.VMEM((max(nz - 1, 1), 6, LANES), F32),
            pltpu.VMEM((2, LANES), F32),
            pltpu.VMEM((ns - 1, 2, LANES), F32),
            pltpu.VMEM((2, LANES), F32),
            pltpu.SemaphoreType.REGULAR,
            pltpu.SemaphoreType.REGULAR,
            dma((groups * integ,)),
            dma((4,)),
            dma((max(nc - 1, 1),)),
            dma((max(nc - 1, 1),)),
            dma((max(nz - 1, 1),)),
            dma((max(nz - 1, 1),)),
            dma((ns - 1,)),
            dma((ns - 1,)),
            dma((3,)),
            dma((3,)),
            dma((ns - 1,)),
            dma((ns - 1,)),
        ],
        compiler_params=pltpu.CompilerParams(
            collective_id=0, has_side_effects=True, vmem_limit_bytes=16 << 20
        ),
    )(*[pltpu.with_memory_space_constraint(v, pltpu.HBM) for v in (
        spectra.reshape(groups, integ // SUB, SUB, rows, LANES).transpose(0, 1, 3, 2, 4),
        channel_gain.reshape(rows, LANES),
        bandpass_bin.reshape(rows, LANES),
        drift_range,
        hit_cutoff,
    )])
    return out.reshape(ns * groups, 1, chans)


def solution(mesh, near_count=8):
    return jax.shard_map(
        functools.partial(shards, near_count),
        mesh=mesh,
        in_specs=(P("section", None, "freq"), P("freq"), P("freq"), P(), P()),
        out_specs=P(None, "section", "freq"),
        check_vma=False,
    )
```

```python
import functools

import jax
import jax.numpy as jnp
from jax import lax
from jax.experimental import pallas as pl
from jax.experimental.pallas import tpu as pltpu
from jax.sharding import PartitionSpec as P

F32 = jnp.float32
BF16 = jnp.bfloat16
LANES = 128
SUB = 8
MESH = pl.DeviceIdType.MESH


def remote(src, dst, send, recv, where):
    return pltpu.make_async_remote_copy(
        src_ref=src, dst_ref=dst, send_sem=send, recv_sem=recv, device_id=where, device_id_type=MESH
    )


def kernel(
    sizes,
    spec_hbm,
    gain_hbm,
    bins_hbm,
    reach_hbm,
    cut_hbm,
    out_ref,
    nat,
    gain,
    bins,
    reach,
    cut,
    halo,
    halo_gain,
    halo_bins,
    factor,
    factor_rows,
    norm,
    quads,
    total,
    scores,
    part,
    near,
    near_sum,
    far,
    far_sum,
    early,
    before,
    far_ready,
    section_ready,
    spec_sem,
    load_sem,
    near_send,
    near_recv,
    far_send,
    far_recv,
    early_send,
    early_recv,
    halo_send,
    halo_recv,
    score_send,
    score_recv,
):
    ns, nf, nc, groups, integ, chans, total_bins = sizes
    nz = nf // nc
    rows = chans // LANES
    wide = groups * rows
    me = lax.axis_index("section")
    here = lax.axis_index("freq")
    z, xc = lax.div(here, nc), lax.rem(here, nc)

    at_end = here == nf - 1
    near_peers = [z * nc + lax.rem(xc + d, nc) for d in range(1, nc)]
    far_peers = [lax.rem(here + d * nc, nf) for d in range(1, nz)]
    section_peers = [lax.rem(me + d, ns) for d in range(1, ns)]
    left, right = lax.rem(here + nf - 1, nf), lax.rem(here + 1, nf)

    loads = [
        pltpu.make_async_copy(bins_hbm, bins, load_sem.at[0]),
        pltpu.make_async_copy(gain_hbm, gain, load_sem.at[1]),
        pltpu.make_async_copy(reach_hbm, reach, load_sem.at[2]),
        pltpu.make_async_copy(cut_hbm.at[pl.ds(groups * me, groups)], cut, load_sem.at[3]),
    ]
    spec_loads = [
        pltpu.make_async_copy(
            spec_hbm.at[g, t // SUB, :, t % SUB, :],
            nat.at[g, t, pl.ds(0, rows)],
            spec_sem.at[g * integ + t],
        )
        for g in range(groups)
        for t in range(integ)
    ]
    for c in loads[:2] + spec_loads:
        c.start()

    barrier = pltpu.get_barrier_semaphore()
    def greet(sem, cond, where):
        @pl.when(cond)
        def _():
            pl.semaphore_signal(sem, inc=1, device_id=where, device_id_type=MESH)

    for d, peer in enumerate(section_peers, 1):
        greet(barrier, me + d < ns, {"section": peer})
    for d, peer in enumerate(far_peers, 1):
        greet(barrier, z + d < nz, {"freq": peer})
    greet(barrier, here < nf - 1, {"freq": right})
    for peer in near_peers:
        pl.semaphore_signal(barrier, inc=1, device_id={"freq": peer}, device_id_type=MESH)

    for c in loads[2:]:
        c.start()
    for c in loads[:2]:
        c.wait()
    bin_row = lax.broadcasted_iota(jnp.int32, (total_bins, LANES), 0).astype(F32).astype(BF16)
    named = bins[...].astype(F32).astype(BF16)
    for c in spec_loads:
        c.wait()
    acc = jnp.zeros((SUB, total_bins), F32)
    for r0 in range(0, rows, SUB):
        span = pl.ds(r0, SUB)
        high, middle, low = [], [], []
        for g in range(groups):
            value = nat[g, 0, span]
            for t in range(1, integ):
                value = value + nat[g, t, span]
            value = value * gain[span]
            high.append(value.astype(BF16).astype(F32))
            value = value - high[-1]
            middle.append(value.astype(BF16).astype(F32))
            low.append(value - middle[-1])
        ones = [jnp.ones((SUB, LANES), F32)] * 2
        turned = jnp.transpose(jnp.stack(high + middle + low + ones), (1, 0, 2))
        lhs = jnp.concatenate([turned[r] for r in range(SUB)], axis=1).astype(BF16)
        one_hot = jnp.concatenate(
            [
                jnp.where(bin_row == named[r : r + 1], jnp.ones((), BF16), jnp.zeros((), BF16))
                for r in range(r0, r0 + SUB)
            ],
            axis=1,
        )
        acc = acc + lax.dot_general(
            lhs,
            one_hot,
            (((1,), (1,)), ((), ())),
            preferred_element_type=F32,
        )
    sums = acc[0:2] + acc[2:4] + acc[4:6]
    counts = acc[6:8]
    tile = jnp.concatenate(
        [sums[:, :LANES], counts[:1, :LANES], sums[:, LANES:], counts[:1, LANES:]], axis=0
    )
    part[...] = tile

    pl.semaphore_wait(barrier, nc - 1 + z + me + jnp.where(here > 0, 1, 0))
    near_copies = [
        remote(part, near.at[d], near_send.at[d], near_recv.at[d], {"freq": p})
        for d, p in enumerate(near_peers)
    ]
    halo_copies = [
        remote(src, dst, halo_send.at[i], halo_recv.at[i], {"freq": left})
        for i, (src, dst) in enumerate(
            [
                (nat.at[:, :, 0], halo),
                (gain.at[pl.ds(0, SUB)], halo_gain),
                (bins.at[pl.ds(0, SUB)], halo_bins),
            ]
        )
    ]
    for c in near_copies:
        c.start()

    for d, peer in enumerate(far_peers, 1):
        greet(far_ready, z + d >= nz, {"freq": peer})
    for d, peer in enumerate(section_peers, 1):
        greet(section_ready, me + d >= ns, {"section": peer})

    @pl.when(here > 0)
    def _():
        for c in halo_copies:
            c.start()

    def turn(t, shift):
        block = jnp.concatenate(
            [nat[g, t, pl.ds(shift, rows)] for g in range(groups)], axis=0
        )
        norm[t, pl.ds(shift * LANES, LANES)] = jnp.transpose(block)

    for t in range(integ):
        turn(t, 0)
    for c in near_copies:
        c.wait_recv()
    near_tile = tile
    for d in range(nc - 1):
        near_tile = near_tile + near[d]
    near_sum[...] = near_tile
    far_copies = [
        remote(near_sum, far.at[d], far_send.at[d], far_recv.at[d], {"freq": p})
        for d, p in enumerate(far_peers)
    ]
    for d, c in enumerate(far_copies, 1):
        pl.when(z + d >= nz)(c.start)

    @pl.when(here < nf - 1)
    def _():
        for c in halo_copies:
            c.wait_recv()

    for g in range(groups):
        for t in range(integ):
            nat[g, t, pl.ds(rows, 1)] = jnp.where(at_end, 1.0, halo[g, t : t + 1])
    for t in range(integ):
        turn(t, 1)

    @pl.when(z < nz - 1)
    def _():
        pl.semaphore_wait(far_ready, nz - 1 - z)

    for d, c in enumerate(far_copies, 1):
        pl.when(z + d < nz)(c.start)
    for c in far_copies:
        c.wait_recv()
    far_tile = near_tile
    for d in range(nz - 1):
        far_tile = far_tile + far[d]
    far_sum[...] = jnp.concatenate(
        [far_tile[0:1] + far_tile[1:2], far_tile[3:4] + far_tile[4:5]], axis=0
    )
    early_copies = [
        remote(far_sum, early.at[d], early_send.at[d], early_recv.at[d], {"section": p})
        for d, p in enumerate(section_peers)
    ]
    @pl.when(me < ns - 1)
    def _():
        pl.semaphore_wait(section_ready, ns - 1 - me)

    for d, c in enumerate(early_copies, 1):
        pl.when(me + d < ns)(c.start)
    before[...] = jnp.zeros((2, LANES), F32)

    for c in loads[2:]:
        c.wait()
    lane = lax.broadcasted_iota(jnp.int32, (SUB, wide), 1)
    for d, c in enumerate(early_copies, 1):

        @pl.when(d <= me)
        def _():
            c.wait_recv()
            before[...] += early[d - 1]

    run_low, run_high = before[0:1], before[1:2]

    def looked_up(at, low, high):
        inner = jnp.bitwise_and(at, LANES - 1)
        return jnp.where(
            at < LANES,
            jnp.take_along_axis(low, inner, axis=1),
            jnp.take_along_axis(high, inner, axis=1),
        )

    for g in range(groups):
        run_low = run_low + far_tile[g : g + 1]
        run_high = run_high + far_tile[3 + g : 4 + g]
        order = (integ * (groups * me + g + 1)).astype(F32)
        low = jnp.broadcast_to(order * far_tile[2:3] / run_low, (SUB, LANES))
        high = jnp.broadcast_to(order * far_tile[5:6] / run_high, (SUB, LANES))
        for r0 in range(0, rows, SUB):
            span = pl.ds(r0, SUB)
            factor[g, span] = gain[span] * looked_up(bins[span], low, high)
        past = halo_gain[...] * looked_up(halo_bins[...], low, high)
        factor[g, pl.ds(rows, SUB)] = jnp.where(at_end, 1.0, past)
    for shift in (0, 1):
        block = jnp.concatenate([factor[g, pl.ds(shift, rows)] for g in range(groups)], axis=0)
        factor_rows[pl.ds(shift * LANES, LANES)] = jnp.transpose(block)

    def score_copy(i, off):
        return remote(
            scores.at[i],
            out_ref.at[pl.ds(groups * me, groups)],
            score_send.at[i],
            score_recv.at[off - 1],
            {"section": lax.rem(me + off, ns)},
        )

    orders = [2042460, 469735, 351974, 1879269, 1893724, 1893675, 1894242, 2053345]
    order = orders[0]
    for section in range(1, ns):
        order = jnp.where(me == section, orders[section], order)

    def one_stride(i, order):
        off = lax.rem(order, ns)
        dst = lax.rem(me + off, ns)
        k = dst + 1
        first_group = lane < rows

        def by_group(values):
            return jnp.where(first_group, values[0], values[1])

        levels = [
            by_group([cut[g, dst, d].astype(F32) * (4.0 / 256.0) + integ for g in range(groups)])
            for d in range(integ)
        ]
        weight = by_group(
            [jnp.where(k <= reach[groups * me + g], 0.25 / integ, 0.0) for g in range(groups)]
        )

        chunk = 4

        def lower(b, inner):
            for c in range(chunk):
                r = pl.multiple_of((b * chunk + c) * SUB, SUB)
                scale = [factor_rows[pl.ds(r + n * k, SUB)] for n in range(4)]
                for q in range(integ // 4):

                    def x(t, n):
                        return norm[4 * q + t, pl.ds(r + n * k, SUB)] * scale[n]

                    x0, x10, x11 = x(0, 0), x(1, 0), x(1, 1)
                    x20, x21, x22 = x(2, 0), x(2, 1), x(2, 2)
                    x30, x31, x32, x33 = x(3, 0), x(3, 1), x(3, 2), x(3, 3)
                    u0, u1 = x0 + x10, x0 + x11
                    span = pl.ds(r, SUB)
                    quads[4 * q, span] = u0 + (x20 + x30)
                    quads[4 * q + 1, span] = u0 + (x21 + x31)
                    quads[4 * q + 2, span] = u1 + (x21 + x32)
                    quads[4 * q + 3, span] = u1 + (x22 + x33)
            return inner

        tall = chunk * SUB
        lax.fori_loop(0, (LANES + 12 * k + tall - 1) // tall, lower, 0)

        def upper(b, inner):
            for c in range(chunk):
                r = pl.multiple_of((b * chunk + c) * SUB, SUB)

                def y(row, n):
                    return quads[row, pl.ds(r + n * k, SUB)]

                sums_over = jnp.zeros((SUB, wide), F32)
                for a in range(integ // 4):
                    own = y(a, 0)
                    for h in (2 * a, 2 * a + 1):
                        e = h - a
                        first = own + y(4 + a, e)
                        for d in (2 * h, 2 * h + 1):
                            n = d - h
                            drift = first + (y(8 + a, n) + y(12 + a, n + e))
                            sums_over = sums_over + jnp.maximum(drift - levels[d], 0.0)
                total[pl.ds(r, SUB)] = sums_over * weight
            return inner

        lax.fori_loop(0, LANES // tall, upper, 0)
        turned = jnp.transpose(total[...])
        for g in range(groups):
            scores[i, g] = turned[g * rows : (g + 1) * rows]

        @pl.when(i < ns - 1)
        def _():
            score_copy(i, off).start()

        return lax.div(order, ns)

    lax.fori_loop(0, ns, one_stride, order)
    kept = pltpu.make_async_copy(
        scores.at[ns - 1], out_ref.at[pl.ds(groups * me, groups)], load_sem.at[0]
    )
    kept.start()
    for c in near_copies + far_copies:
        c.wait_send()

    @pl.when(here > 0)
    def _():
        for c in halo_copies:
            c.wait_send()

    for d, c in enumerate(early_copies, 1):
        pl.when(me + d < ns)(c.wait_send)
    for i in range(ns - 1):
        score_copy(i, i + 1).wait_recv()
    kept.wait()
    for i in range(ns - 1):
        score_copy(i, i + 1).wait_send()


def shards(near_count, spectra, channel_gain, bandpass_bin, drift_range, hit_cutoff):
    groups, integ, chans = spectra.shape
    ns, nf = lax.axis_size("section"), lax.axis_size("freq")
    total_bins = 2 * LANES
    nc, nz = near_count, nf // near_count
    rows = chans // LANES
    wide = groups * rows
    sizes = (ns, nf, nc, groups, integ, chans, total_bins)
    dma = pltpu.SemaphoreType.DMA
    tile = (SUB, LANES)
    out = pl.pallas_call(
        functools.partial(kernel, sizes),
        out_shape=jax.ShapeDtypeStruct((ns * groups, rows, LANES), F32),
        in_specs=[pl.BlockSpec(memory_space=pltpu.HBM)] * 5,
        out_specs=pl.BlockSpec(memory_space=pl.ANY),
        scratch_shapes=[
            pltpu.VMEM((groups, integ, rows + SUB, LANES), F32),
            pltpu.VMEM((rows, LANES), F32),
            pltpu.VMEM((rows, LANES), jnp.int32),
            pltpu.SMEM((ns * groups,), jnp.int32),
            pltpu.SMEM((groups, *hit_cutoff.shape[1:]), jnp.int32),
            pltpu.VMEM((groups, integ, LANES), F32),
            pltpu.VMEM(tile, F32),
            pltpu.VMEM(tile, jnp.int32),
            pltpu.VMEM((groups, rows + SUB, LANES), F32),
            pltpu.VMEM((2 * LANES, wide), F32),
            pltpu.VMEM((integ, 2 * LANES + SUB, wide), F32),
            pltpu.VMEM((integ, 2 * LANES + SUB, wide), F32),
            pltpu.VMEM((LANES, wide), F32),
            pltpu.VMEM((ns, groups, rows, LANES), F32),
            pltpu.VMEM((6, LANES), F32),
            pltpu.VMEM((max(nc - 1, 1), 6, LANES), F32),
            pltpu.VMEM((6, LANES), F32),
            pltpu.VMEM((max(nz - 1, 1), 6, LANES), F32),
            pltpu.VMEM((2, LANES), F32),
            pltpu.VMEM((ns - 1, 2, LANES), F32),
            pltpu.VMEM((2, LANES), F32),
            pltpu.SemaphoreType.REGULAR,
            pltpu.SemaphoreType.REGULAR,
            dma((groups * integ,)),
            dma((4,)),
            dma((max(nc - 1, 1),)),
            dma((max(nc - 1, 1),)),
            dma((max(nz - 1, 1),)),
            dma((max(nz - 1, 1),)),
            dma((ns - 1,)),
            dma((ns - 1,)),
            dma((3,)),
            dma((3,)),
            dma((ns - 1,)),
            dma((ns - 1,)),
        ],
        compiler_params=pltpu.CompilerParams(
            collective_id=0, has_side_effects=True, vmem_limit_bytes=16 << 20
        ),
    )(*[pltpu.with_memory_space_constraint(v, pltpu.HBM) for v in (
        spectra.reshape(groups, integ // SUB, SUB, rows, LANES).transpose(0, 1, 3, 2, 4),
        channel_gain.reshape(rows, LANES),
        bandpass_bin.reshape(rows, LANES),
        drift_range,
        hit_cutoff,
    )])
    return out.reshape(ns * groups, 1, chans)


def solution(mesh, near_count=8):
    return jax.shard_map(
        functools.partial(shards, near_count),
        mesh=mesh,
        in_specs=(P("section", None, "freq"), P("freq"), P("freq"), P(), P()),
        out_specs=P(None, "section", "freq"),
        check_vma=False,
    )
```
